128 devices in a mesh: rep: 16 (over z_lo, y, core), tp: 8 (over z_hi, x).
Axes of the slice: x: 4, y: 4, z: 4 (z_hi: 2, z_lo: 2; z = z_hi * 2 + z_lo), core: 2. Of those that a mesh axis runs over, the one named last changes fastest.
Arguments:
- residual_in: bfloat16 [16, 512, 8192], P('rep', 'tp'), may hold values from -6 to 6
- norm_gain: bfloat16 [8192], replicated, may hold values from 0.099609375 to 1.8984375
- w_query: bfloat16 [8192, 4096], P(None, 'tp'), may hold values from -1 to 1
- w_keyval: bfloat16 [8192, 1024], P(None, 'tp'), may hold values from -0.0625 to 0.0625
- w_out: bfloat16 [4096, 8192], P('tp'), may hold values from -0.375 to 0.375
- score_head: bfloat16 [8192], replicated, may hold values from -0.0625 to 0.0625
- lengths: int32 [16], P('rep'), may hold values from 256 to 512
- policy_slots: bfloat16 [16, 768, 8192], P('rep', None, 'tp'), may hold values from -6 to 6
Outputs:
- scored_hidden: bfloat16 [16, 512, 8192], P('rep', 'tp')
- rewards: float32 [16], P('rep')
- policy_copies: bfloat16 [16, 768, 8192], P('rep', None, 'tp')
The draws below stay inside these ranges and needn't reach their ends.
All inputs are finite; a program needn't handle non-finite values.
Results may differ from the reference program's by a relative error of at most 0.017.
The reference program's roundings to bfloat16 on the way count: a program that leaves them out, or rounds other values in their place, can miss the bound.
Values may be sent and summed in bfloat16 or wider, within the bound.
A program may use at most 128 MiB of HBM per device.

```python
import jax
import jax.numpy as jnp
from jax import lax

D = 8192
QH = 32
KVH = 4
HS = 128
LEN = 512
PROWS = 768
QW = 4096
KW = 512
REPLICAS = 16
N_TP = 8


def draw_w_query(key, part):
    values = jax.random.normal(jax.random.fold_in(key, 11), (D, QW), jnp.float32) * D ** (-0.5)
    return jnp.clip(values, -1.0, 1.0).astype(jnp.bfloat16)


def with_ends(result, own_key, low, largest):
    longest = result.shape.index(max(result.shape))
    spots = []
    for shift in (0, 1):
        where = [jax.random.randint(jax.random.fold_in(own_key, axis), (), 0, length) for axis, length in enumerate(result.shape)]
        where[longest] = (where[longest] + shift) % result.shape[longest]
        spots.append(tuple(where))
    return result.at[spots[0]].set(low).at[spots[1]].set(largest)


def block_levels(rng, dims, pieces, least, largest):
    gain, own = 1.0, jax.random.fold_in(rng, 6)
    for position, blocks in pieces:
        draws = jnp.exp(jax.random.uniform(jax.random.fold_in(own, position), (blocks,), jnp.float32, least / len(pieces), largest / len(pieces)))
        gain = gain * jnp.repeat(draws, dims[position] // blocks).reshape([-1 if axis == position else 1 for axis in range(len(dims))])
    return gain


def centred(rng, dims, deviation, bound, cuts=(), held_as=jnp.bfloat16):
    result = jax.random.normal(rng, dims, jnp.float32) * deviation
    if len(cuts) > 0:
        result = block_levels(rng, dims, cuts, -0.22, 0.18) * result
    return jnp.clip(result, min=-bound, max=bound).astype(held_as)


def setup_inputs(seed: int = 0) -> dict:
    arg_keys = jax.random.split(jax.random.key(seed), 9)
    residual_in = centred(arg_keys[0], (REPLICAS, LEN, D), 1.0, 6.0, ((0, 16), (1, 8)))
    norm_gain = jnp.clip(1.0 + 0.18 * jax.random.normal(arg_keys[1], (D,), jnp.float32), 0.099609375, 1.8984375).astype(jnp.bfloat16)
    w_query = draw_w_query(jax.random.fold_in(arg_keys[8], 71), 0)
    w_keyval = centred(arg_keys[3], (D, 2 * KW), D ** -0.5, 0.0625, ((1, 8),))
    w_out = centred(arg_keys[4], (QW, D), (QW // 16) ** -0.5, 0.375, ((0, 8),))
    score_head = centred(arg_keys[5], (D,), D ** -0.5, 0.0625)
    lengths = with_ends(jax.random.randint(arg_keys[6], (REPLICAS,), LEN // 2, LEN + 1), jax.random.fold_in(arg_keys[6], 1), LEN // 2, LEN).astype(jnp.int32)
    policy_slots = centred(arg_keys[7], (REPLICAS, PROWS, D), 1.0, 6.0, ((0, 16), (2, 8)))
    return dict(residual_in=residual_in, norm_gain=norm_gain, w_query=w_query, w_keyval=w_keyval, w_out=w_out, score_head=score_head, lengths=lengths, policy_slots=policy_slots)


def one_rollout(residual_row, length, norm_gain, w_query, w_keyval, w_out, score_head):
    resid = residual_row.astype(jnp.float32)
    meansq = lax.optimization_barrier(jnp.mean(resid * resid, axis=-1, keepdims=True))
    normed = (resid * lax.rsqrt(meansq + 1e-05) * norm_gain.astype(jnp.float32)).astype(jnp.bfloat16)
    queries = jnp.dot(normed, w_query, preferred_element_type=jnp.float32).astype(jnp.bfloat16)
    keyvals = jnp.dot(normed, w_keyval, preferred_element_type=jnp.float32).astype(jnp.bfloat16)
    group = QH // KVH
    qheads = queries.reshape(LEN, QH, HS).transpose(1, 0, 2).astype(jnp.float32)
    kheads = keyvals[:, :KW].reshape(LEN, KVH, HS).transpose(1, 0, 2)
    vheads = keyvals[:, KW:].reshape(LEN, KVH, HS).transpose(1, 0, 2)
    kheads = jnp.repeat(kheads, group, axis=0).astype(jnp.float32)
    vheads = jnp.repeat(vheads, group, axis=0).astype(jnp.float32)
    scores = jnp.einsum('hqd,hkd->hqk', qheads, kheads) * HS ** (-0.5)
    rowpos = jnp.arange(LEN, dtype=jnp.int32)[:, None]
    colpos = jnp.arange(LEN, dtype=jnp.int32)[None, :]
    valid = (colpos <= rowpos) & (colpos < length)
    scores = jnp.where(valid[None], scores, -1e+30)
    probs = jax.nn.softmax(scores, axis=-1).astype(jnp.bfloat16)
    attended = jnp.einsum('hqk,hkd->hqd', probs.astype(jnp.float32), vheads).astype(jnp.bfloat16)
    attended = attended.transpose(1, 0, 2).reshape(LEN, QW)
    groups = attended.reshape(LEN, N_TP, QW // N_TP).astype(jnp.float32)
    wgroups = w_out.reshape(N_TP, QW // N_TP, D).astype(jnp.float32)
    partial_value = jnp.einsum('lti,tid->tld', groups, wgroups).astype(jnp.bfloat16)
    partial_value = lax.optimization_barrier(partial_value)
    summed = lax.optimization_barrier(jnp.sum(partial_value.astype(jnp.float32), axis=0))
    hidden = (resid + summed).astype(jnp.bfloat16)
    head = score_head.astype(jnp.float32)
    last_row = lax.dynamic_slice_in_dim(hidden, (length - 1).astype(jnp.int32), 1, 0)[0]
    reward = jnp.sum(last_row.astype(jnp.float32) * head)
    pooled = jnp.sum(hidden.astype(jnp.float32) * head[None, :]) * LEN ** (-0.5)
    return (hidden, reward + pooled)

def reference(residual_in, norm_gain, w_query, w_keyval, w_out, score_head, lengths, policy_slots):

    def step(pair):
        return one_rollout(pair[0], pair[1], norm_gain, w_query, w_keyval, w_out, score_head)
    scored_hidden, rewards = lax.map(step, (residual_in, lengths.astype(jnp.int32)))
    policy_copies = jnp.broadcast_to(policy_slots[0:1], policy_slots.shape)
    return (scored_hidden, rewards.astype(jnp.float32), policy_copies)
```

```python
import functools

import jax
import jax.numpy as jnp
from jax import lax
from jax.experimental import pallas as pl
from jax.experimental.pallas import tpu as pltpu
from jax.sharding import PartitionSpec as P

HS = 128
N = 8
D = 8192
CW = D // N
ROWS = 64
PLANE = 256
QC = 512
WC = QC + 128
PCH = 8
LAG = 1
MESH = pl.DeviceIdType.MESH
BF = jnp.bfloat16
F32 = jnp.float32


def rcopy(src, dst, ssem, rsem, dev):
    return pltpu.make_async_remote_copy(
        src_ref=src, dst_ref=dst, send_sem=ssem, recv_sem=rsem, device_id=dev, device_id_type=MESH
    )


def when_in(value, low, high, fn):
    @pl.when((value >= low) & (value < high))
    def _():
        fn(value)


class Place:
    def __init__(self):
        rep = lax.axis_index("rep")
        tp = lax.axis_index("tp")
        self.rep, self.tp = rep, tp
        self.core = core = lax.rem(rep, 2)
        self.y = y = lax.rem(rep // 2, 4)
        self.zl = zl = rep // 8
        self.x = x = lax.rem(tp, 4)
        self.zh = zh = tp // 4
        self.xp, self.xm, self.xo = lax.rem(x + 1, 4), lax.rem(x + 3, 4), lax.rem(x + 2, 4)
        self.yp, self.ym, self.yo = lax.rem(y + 1, 4), lax.rem(y + 3, 4), lax.rem(y + 2, 4)
        self.xr = (rep, zh * 4 + self.xp)
        self.xl = (rep, zh * 4 + self.xm)
        self.yr = ((zl * 4 + self.yp) * 2 + core, tp)
        self.yl = ((zl * 4 + self.ym) * 2 + core, tp)
        self.cross = (((1 - zl) * 4 + y) * 2 + core, (1 - zh) * 4 + x)
        self.zpart = (((1 - zl) * 4 + y) * 2 + core, tp)
        self.sib = (rep + 1 - 2 * core, tp)


class Exchange:
    def __init__(self, p, near, far, rows, sems):
        self.p, self.near, self.far, self.rows = p, near, far, rows
        (self.cs, self.cr, self.y1s, self.y1r, self.y2s, self.y2r, self.zs, self.zr, self.ds, self.dr) = sems

    def piece(self, yy, core, part=0, parts=1):
        size = self.rows // 8 // parts
        start = yy * (self.rows // 4) + core * (self.rows // 8) + part * size
        return pl.ds(pl.multiple_of(start, 16), size)

    def move(self, k, where, ssem, rsem, dev):
        ref = self.far.at[k, where]
        return rcopy(ref, ref, ssem, rsem, dev)

    def over_z(self, k):
        p = self.p
        where = self.piece(p.y, p.core)
        return rcopy(self.near.at[k, where], self.far.at[k, where], self.cs.at[k], self.cr.at[k], p.cross)

    def along_y(self, d, k):
        p = self.p
        return self.move(k, self.piece(p.y, p.core), self.y1s.at[d, k], self.y1r.at[d, k], p.yl if d else p.yr)

    def along_y_in(self, d, k):
        p = self.p
        return self.move(k, self.piece(p.yp if d else p.ym, p.core), self.y1s.at[d, k], self.y1r.at[d, k], p.sib)

    def onward_y(self, d, k):
        p = self.p
        where = self.piece(p.yp if d else p.ym, p.core, 2 * p.zl + d, 4)
        return self.move(k, where, self.y2s.at[d, k], self.y2r.at[d, k], p.yl if d else p.yr)

    def onward_y_in(self, d, k):
        p = self.p
        where = self.piece(p.yo, p.core, 2 * p.zl + d, 4)
        return self.move(k, where, self.y2s.at[d, k], self.y2r.at[d, k], p.sib)

    def to_zpart(self, k):
        p = self.p
        return self.move(k, self.piece(p.yo, p.core, p.zl, 2), self.zs.at[k], self.zr.at[k], p.zpart)

    def to_zpart_in(self, k):
        p = self.p
        return self.move(k, self.piece(p.yo, p.core, 1 - p.zl, 2), self.zs.at[k], self.zr.at[k], p.zpart)

    def to_sib(self, j, k, core):
        p = self.p
        where = (
            self.piece(p.y, core),
            self.piece(p.ym, core),
            self.piece(p.yp, core),
            self.piece(p.yo, core, p.zl, 2),
            self.piece(p.yo, core, 1 - p.zl, 2),
        )[j]
        return self.move(k, where, self.ds.at[j, k], self.dr.at[j, k], p.sib)

    def stage0(self, k):
        self.over_z(k).wait_recv()
        for d in (0, 1):
            self.along_y(d, k).start()
        self.to_sib(0, k, self.p.core).start()

    def stage1(self, k):
        for d in (0, 1):
            self.along_y_in(d, k).wait_recv()
            self.onward_y(d, k).start()
            self.to_sib(1 + d, k, self.p.core).start()

    def stage2(self, k):
        for d in (0, 1):
            self.onward_y_in(d, k).wait_recv()
        self.to_zpart(k).start()
        self.to_sib(3, k, self.p.core).start()

    def stage3(self, k):
        self.to_zpart_in(k).wait_recv()
        self.to_sib(4, k, self.p.core).start()

    def ready(self, k):
        for j in range(5):
            self.to_sib(j, k, 1 - self.p.core).wait_recv()

    def drain(self, k):
        self.over_z(k).wait_send()
        for d in (0, 1):
            self.along_y(d, k).wait_send()
            self.onward_y(d, k).wait_send()
        self.to_zpart(k).wait_send()
        for j in range(5):
            self.to_sib(j, k, self.p.core).wait_send()

    def stages(self, i):
        for s, stage in enumerate((self.stage0, self.stage1, self.stage2, self.stage3)):
            when_in(i - s, 0, N, stage)


def kernel(
    gain, head, length, resid_h, wq_h, wkv_h, wo_h, pol_h,
    hid_o, rew_o, pol_o,
    rv, tok, wl, wr, ol, fr, acc, qv, kvs, kva, att, part, r1, r2, hid, racc, rsend, rrecv, pol,
    lsem, wsem, osem, t1s, t1r, t2s, t2r,
    acs, acr, ay1s, ay1r, ay2s, ay2r, azs, azr, ads, adr,
    bcs, bcr, by1s, by1r, by2s, by2r, bzs, bzr, bds, bdr,
    ks, kr, s1s, s1r, s2s, s2r, hsem, ws, wrs, ps, pr, psem,
):
    p = Place()
    ea = Exchange(p, wl, wr, CW, (acs, acr, ay1s, ay1r, ay2s, ay2r, azs, azr, ads, adr))
    eb = Exchange(p, ol, fr, 512, (bcs, bcr, by1s, by1r, by2s, by2r, bzs, bzr, bds, bdr))

    barrier = pltpu.get_barrier_semaphore()
    for t in range(8):
        @pl.when(t != p.tp)
        def _():
            pl.semaphore_signal(barrier, inc=1, device_id=(p.rep, t), device_id_type=MESH)
    for dev in (p.yr, p.yl, p.cross, p.zpart, p.sib):
        pl.semaphore_signal(barrier, inc=1, device_id=dev, device_id_type=MESH)

    def load_resid(k):
        return pltpu.make_async_copy(resid_h.at[:, pl.ds(k * CW, CW)], rv.at[k], lsem.at[k])

    def load_wq(k):
        at = pl.ds(pl.multiple_of(k * CW, CW), CW)
        return pltpu.make_async_copy(wq_h.at[at], wl.at[k, :, pl.ds(0, QC)], wsem.at[0, k])

    def load_wkv(k):
        at = pl.ds(pl.multiple_of(k * CW, CW), CW)
        return pltpu.make_async_copy(wkv_h.at[at], wl.at[k, :, pl.ds(QC, 128)], wsem.at[1, k])

    def load_wo(k):
        at = pl.ds(pl.multiple_of(k * CW, CW), CW)
        return pltpu.make_async_copy(wo_h.at[:, at], ol.at[k], osem.at[k])

    root = (p.zl == 0) & (p.y == 0) & (p.core == 0)
    load_pol = pltpu.make_async_copy(pol_h, pol, psem)

    for k in range(N):
        load_resid(k).start()

    @pl.loop(0, N)
    def _(k):
        load_wq(k).start()
        load_wkv(k).start()

    @pl.loop(0, N)
    def _(k):
        load_wo(k).start()

    @pl.when(root)
    def _():
        load_pol.start()

    own = pl.ds(pl.multiple_of(p.x * ROWS, ROWS), ROWS)
    squares = jnp.zeros((ROWS, 1), F32)
    for k in range(N):
        load_resid(k).wait()
        r = rv[k].astype(F32)
        squares += jnp.sum(r * r, axis=-1, keepdims=True)
    scale = lax.rsqrt(squares / D + 1e-05)
    for k in range(N):
        tok[k, own, :] = (rv[k].astype(F32) * scale * gain[:, k * CW : (k + 1) * CW].astype(F32)).astype(BF)

    pl.semaphore_wait(barrier, 12)

    def block(xx, start=0, size=ROWS):
        return pl.ds(pl.multiple_of(xx * ROWS + start, 16), size)

    def token_copy(k, where, ssem, rsem, d):
        ref = tok.at[k, where]
        return rcopy(ref, ref, ssem.at[d, k], rsem.at[d, k], p.xl if d else p.xr)

    def token_out(d, k):
        return token_copy(k, block(p.x), t1s, t1r, d)

    def token_in(d, k):
        return token_copy(k, block(p.xp if d else p.xm), t1s, t1r, d)

    def token_onward(d, k):
        return token_copy(k, block(p.xp if d else p.xm, 32 * d, 32), t2s, t2r, d)

    def token_onward_in(d, k):
        return token_copy(k, block(p.xo, 32 * d, 32), t2s, t2r, d)

    def tokens_send(k):
        for d in (0, 1):
            token_out(d, k).start()

    def tokens_forward(k):
        for d in (0, 1):
            token_in(d, k).wait_recv()
            token_onward(d, k).start()

    @pl.loop(0, N)
    def _(k):
        load_wq(k).wait()
        load_wkv(k).wait()
        ea.over_z(k).start()

    for k in range(2):
        tokens_send(k)

    acc[...] = jnp.zeros_like(acc)

    def project(k):
        for d in (0, 1):
            token_onward_in(d, k).wait_recv()
        ea.ready(k)
        acc[p.zh] = acc[p.zh] + jnp.dot(tok[k], wl[k], preferred_element_type=F32)
        acc[1 - p.zh] = acc[1 - p.zh] + jnp.dot(tok[k], wr[k], preferred_element_type=F32)

    def open_b(k):
        load_wo(k).wait()
        eb.over_z(k).start()

    @pl.loop(0, N + 4)
    def _(i):
        when_in(i, 0, N, open_b)
        when_in(i + 2, 0, N, tokens_send)
        when_in(i - 1, 0, N, tokens_forward)
        ea.stages(i)
        eb.stages(i - N)
        when_in(i - 4, 0, N, project)

    kvs[:, 0:HS] = acc[0, :, QC:].astype(BF)
    kvs[:, HS:] = acc[1, :, QC:].astype(BF)
    slot = p.x // 2
    here = pl.ds(pl.multiple_of(p.zh * PLANE, PLANE), PLANE)

    def kv_copy(i):
        xd, zd = 2 * lax.rem(p.x, 2) + i // 2, i % 2
        to = zd * 4 + xd
        return to, rcopy(kvs, kva.at[slot, here], ks.at[i], kr.at[slot * 2 + p.zh], (p.rep, to))

    for i in range(4):
        to, copy = kv_copy(i)

        @pl.when(to != p.tp)
        def _():
            copy.start()

        @pl.when(to == p.tp)
        def _():
            kva[slot, here, :] = kvs[...]

    for s in (0, 1):
        qv[s] = acc[s, :, :QC].astype(BF)
    eb.stages(jnp.int32(4))
    for j in (0, 1):
        for pz in (0, 1):
            @pl.when(pz * 4 + 2 * j + p.x // 2 != p.tp)
            def _():
                ref = kva.at[j, pl.ds(pz * PLANE, PLANE)]
                rcopy(ref, ref, ks.at[0], kr.at[j * 2 + pz], p.sib).wait_recv()

    rowpos = lax.broadcasted_iota(jnp.int32, (PLANE, 512), 0) + p.zh * PLANE
    colpos = lax.broadcasted_iota(jnp.int32, (PLANE, 512), 1)
    last = length[0]
    valid = (colpos <= rowpos) & (colpos < last)
    for s in (0, 1):
        for h in range(4):
            cols = slice(h * HS, (h + 1) * HS)
            scores = lax.dot_general(
                qv[s, :, cols], kva[s, :, 0:HS], (((1,), (1,)), ((), ())), preferred_element_type=F32
            ) * HS ** (-0.5)
            scores = jnp.where(valid, scores, -1e30)
            top = jnp.max(scores, axis=-1, keepdims=True)
            weight = jnp.exp(scores - top)
            probs = (weight / jnp.sum(weight, axis=-1, keepdims=True)).astype(BF)
            att[s, :, cols] = jnp.dot(probs, kva[s, :, HS:], preferred_element_type=F32).astype(BF)
        eb.stages(jnp.int32(5 + s))

    HALF = CW // 2

    def half_copy(d, c):
        src = part.at[c, block(p.xo), pl.ds(d * HALF, HALF)]
        return rcopy(src, r1.at[d, c], s1s.at[d, c], s1r.at[d, c], p.xl if d else p.xr)

    def full_copy(d, c):
        src = part.at[c, block(p.xm if d else p.xp)]
        return rcopy(src, r2.at[d, c], s2s.at[d, c], s2r.at[d, c], p.xl if d else p.xr)

    def hid_copy(c):
        at = pl.ds(pl.multiple_of(c * CW, CW), CW)
        return pltpu.make_async_copy(hid.at[c], hid_o.at[:, at], hsem.at[c])

    def out_project(c):
        eb.ready(c)
        part[c] = (
            jnp.dot(att[p.zh], ol[c], preferred_element_type=F32)
            + jnp.dot(att[1 - p.zh], fr[c], preferred_element_type=F32)
        ).astype(BF)
        for d in (0, 1):
            half_copy(d, c).start()

    def pass_on(c):
        for d in (0, 1):
            half_copy(d, c).wait_recv()
            rows, cols = block(p.xm if d else p.xp), pl.ds(d * HALF, HALF)
            part[c, rows, cols] = (part[c, rows, cols].astype(F32) + r1[d, c].astype(F32)).astype(BF)
            full_copy(d, c).start()

    def finish(c):
        for d in (0, 1):
            full_copy(d, c).wait_recv()
        summed = part[c, own, :].astype(F32) + r2[0, c].astype(F32) + r2[1, c].astype(F32)
        out = (rv[c].astype(F32) + summed).astype(BF)
        hid[c] = out
        racc[...] = racc[...] + out.astype(F32) * head[:, pl.ds(pl.multiple_of(c * CW, CW), CW)].astype(F32)
        hid_copy(c).start()

    first = (p.zl == 0) & (p.core == 0)

    def pol_copy(way, m, dev):
        return rcopy(pol.at[m], pol.at[m], ps.at[way, m], pr.at[m], dev)

    def pol_fan(m):
        pol_copy(1, m, p.zpart).start()
        pol_copy(2, m, p.sib).start()

    ups = p.y < 3
    downs = (p.y == 0) | (p.y > 1)
    hops = (p.y, lax.rem(4 - p.y, 4))

    def pol_step(it):
        @pl.when(root & (it == 0))
        def _():
            load_pol.wait()
            for m in range(4):
                pol_copy(0, m, p.yr).start()
                pol_copy(0, 4 + m, p.yl).start()
            for m in range(PCH):
                pol_fan(m)

        for d in (0, 1):
            m = it - LAG * hops[d]

            @pl.when(first & (p.y > 0) & (m >= 0) & (m < 4))
            def _():
                pol_copy(0, 4 * d + m, p.yr).wait_recv()

                @pl.when(downs if d else ups)
                def _():
                    pol_copy(0, 4 * d + m, p.yl if d else p.yr).start()

                pol_fan(4 * d + m)

            m2 = m - LAG

            @pl.when((p.zl == 1) & (p.core == 0) & (m2 >= 0) & (m2 < 4))
            def _():
                pol_copy(1, 4 * d + m2, p.zpart).wait_recv()
                pol_copy(2, 4 * d + m2, p.sib).start()

    racc[...] = jnp.zeros_like(racc)

    @pl.loop(0, max(N + 2, 4 * LAG + 4))
    def _(it):
        eb.stages(it + 7)
        when_in(it, 0, N, out_project)
        when_in(it - 1, 0, N, pass_on)
        when_in(it - 2, 0, N, finish)
        pol_step(it)

    @pl.when(p.core == 1)
    def _():
        for m in range(PCH):
            pol_copy(2, m, p.sib).wait_recv()

    store_pol = pltpu.make_async_copy(pol, pol_o, psem)
    store_pol.start()

    rows = jnp.sum(racc[...], axis=-1, keepdims=True)
    position = lax.broadcasted_iota(jnp.int32, (ROWS, 1), 0) + p.tp * ROWS
    picked = jnp.where(position == last - 1, 1.0, 0.0) + 512 ** (-0.5)
    share = jnp.sum(rows * picked, axis=0, keepdims=True)
    rsend[...] = jnp.broadcast_to(share, (8, 128))

    def reward_copy(t):
        return rcopy(rsend, rrecv.at[p.tp], ws.at[t], wrs.at[p.tp], (p.rep, t))

    for t in range(8):
        @pl.when(t != p.tp)
        def _():
            reward_copy(t).start()

    @pl.loop(0, N)
    def _(k):
        ea.drain(k)
        eb.drain(k)
        for d in (0, 1):
            token_out(d, k).wait_send()
            token_onward(d, k).wait_send()
            half_copy(d, k).wait_send()
            full_copy(d, k).wait_send()
        hid_copy(k).wait()

    for i in range(4):
        to, copy = kv_copy(i)

        @pl.when(to != p.tp)
        def _():
            copy.wait_send()

    for m in range(PCH):
        @pl.when(first & (downs if m >= 4 else ups))
        def _():
            pol_copy(0, m, p.yr).wait_send()

        @pl.when(first)
        def _():
            pol_copy(1, m, p.zpart).wait_send()

        @pl.when(p.core == 0)
        def _():
            pol_copy(2, m, p.sib).wait_send()

    total = jnp.zeros((8, 128), F32)
    for t in range(8):
        @pl.when(t != p.tp)
        def _():
            rcopy(rsend, rrecv.at[t], ws.at[t], wrs.at[t], (p.rep, t)).wait_recv()
            reward_copy(t).wait_send()

        @pl.when(t == p.tp)
        def _():
            rrecv[t] = rsend[...]

        total += rrecv[t]
    rew_o[...] = total
    store_pol.wait()


def on_device(residual_in, norm_gain, w_query, w_keyval, w_out, score_head, lengths, policy_slots):
    vmem = pl.BlockSpec(memory_space=pltpu.VMEM)
    smem = pl.BlockSpec(memory_space=pltpu.SMEM)
    hbm = pl.BlockSpec(memory_space=pl.ANY)
    dma = pltpu.SemaphoreType.DMA

    def exchange_sems():
        return [dma((N,)), dma((N,)), dma((2, N)), dma((2, N)), dma((2, N)), dma((2, N)),
                dma((N,)), dma((N,)), dma((5, N)), dma((5, N))]

    prow = policy_slots.shape[1]
    hidden, reward, policy = pl.pallas_call(
        kernel,
        out_shape=(
            jax.ShapeDtypeStruct((ROWS, D), BF),
            jax.ShapeDtypeStruct((8, 128), F32),
            jax.ShapeDtypeStruct((PCH, prow // PCH, 1024), BF),
        ),
        in_specs=[vmem, vmem, smem, hbm, hbm, hbm, hbm, hbm],
        out_specs=(hbm, vmem, hbm),
        scratch_shapes=[
            pltpu.VMEM((N, ROWS, CW), BF),
            pltpu.VMEM((N, PLANE, CW), BF),
            pltpu.VMEM((N, CW, WC), BF),
            pltpu.VMEM((N, CW, WC), BF),
            pltpu.VMEM((N, 512, CW), BF),
            pltpu.VMEM((N, 512, CW), BF),
            pltpu.VMEM((2, PLANE, WC), F32),
            pltpu.VMEM((2, PLANE, QC), BF),
            pltpu.VMEM((PLANE, 2 * HS), BF),
            pltpu.VMEM((2, 2 * PLANE, 2 * HS), BF),
            pltpu.VMEM((2, PLANE, QC), BF),
            pltpu.VMEM((N, PLANE, CW), BF),
            pltpu.VMEM((2, N, ROWS, CW // 2), BF),
            pltpu.VMEM((2, N, ROWS, CW), BF),
            pltpu.VMEM((N, ROWS, CW), BF),
            pltpu.VMEM((ROWS, CW), F32),
            pltpu.VMEM((8, 128), F32),
            pltpu.VMEM((8, 8, 128), F32),
            pltpu.VMEM((PCH, prow // PCH, 1024), BF),
            dma((N,)), dma((2, N)), dma((N,)),
            dma((2, N)), dma((2, N)), dma((2, N)), dma((2, N)),
            *exchange_sems(),
            *exchange_sems(),
            dma((4,)), dma((4,)),
            dma((2, N)), dma((2, N)), dma((2, N)), dma((2, N)),
            dma((N,)), dma((8,)), dma((8,)), dma((3, PCH)), dma((PCH,)), dma,
        ],
        compiler_params=pltpu.CompilerParams(
            collective_id=0, has_side_effects=True, vmem_limit_bytes=66_000_000
        ),
        name="block",
    )(
        norm_gain.reshape(1, D), score_head.reshape(1, D), lengths,
        residual_in[0], w_query, w_keyval, w_out, policy_slots[0].reshape(PCH, prow // PCH, 1024),
    )
    return hidden[None], reward[0, :1], policy.reshape(1, prow, 1024)


def solution(mesh):
    placed = (
        P("rep", "tp", None),
        P(),
        P(None, "tp"),
        P(None, "tp"),
        P("tp", None),
        P(),
        P("rep"),
        P("rep", None, "tp"),
    )
    return jax.shard_map(
        on_device,
        mesh=mesh,
        in_specs=placed,
        out_specs=(P("rep", "tp", None), P("rep"), P("rep", None, "tp")),
        check_vma=False,
    )
```

```python
import functools

import jax
import jax.numpy as jnp
from jax import lax
from jax.experimental import pallas as pl
from jax.experimental.pallas import tpu as pltpu
from jax.sharding import PartitionSpec as P

HS = 128
N = 16
D = 8192
CW = D // N
ROWS = 64
PLANE = 256
QC = 512
WC = QC + 128
PCH = 8
LAG = 3
MESH = pl.DeviceIdType.MESH
BF = jnp.bfloat16
F32 = jnp.float32


def rcopy(src, dst, ssem, rsem, dev):
    return pltpu.make_async_remote_copy(
        src_ref=src, dst_ref=dst, send_sem=ssem, recv_sem=rsem, device_id=dev, device_id_type=MESH
    )


def when_in(value, low, high, fn):
    @pl.when((value >= low) & (value < high))
    def _():
        fn(value)


class Place:
    def __init__(self):
        rep = lax.axis_index("rep")
        tp = lax.axis_index("tp")
        self.rep, self.tp = rep, tp
        self.core = core = lax.rem(rep, 2)
        self.y = y = lax.rem(rep // 2, 4)
        self.zl = zl = rep // 8
        self.x = x = lax.rem(tp, 4)
        self.zh = zh = tp // 4
        self.xp, self.xm, self.xo = lax.rem(x + 1, 4), lax.rem(x + 3, 4), lax.rem(x + 2, 4)
        self.yp, self.ym, self.yo = lax.rem(y + 1, 4), lax.rem(y + 3, 4), lax.rem(y + 2, 4)
        self.xr = (rep, zh * 4 + self.xp)
        self.xl = (rep, zh * 4 + self.xm)
        self.yr = ((zl * 4 + self.yp) * 2 + core, tp)
        self.yl = ((zl * 4 + self.ym) * 2 + core, tp)
        self.cross = (((1 - zl) * 4 + y) * 2 + core, (1 - zh) * 4 + x)
        self.zpart = (((1 - zl) * 4 + y) * 2 + core, tp)
        self.sib = (rep + 1 - 2 * core, tp)


class Exchange:
    def __init__(self, p, near, far, rows, sems):
        self.p, self.near, self.far, self.rows = p, near, far, rows
        self.sent, self.cr, self.y1r, self.y2r, self.z1r, self.z2r, self.dr = sems

    def piece(self, yy, core, sub=0, subs=4):
        size = self.rows // 32
        start = yy * (self.rows // 4) + core * (self.rows // 8) + sub * size
        return pl.ds(pl.multiple_of(start, 16), subs * size)

    def move(self, k, where, rsem, dev):
        ref = self.far.at[k, where]
        rcopy(ref, ref, self.sent, rsem.at[k], dev).start()

    def arrived(self, k, count, rsem):
        ref = self.far.at[k, pl.ds(0, count * (self.rows // 32))]
        rcopy(ref, ref, self.sent, rsem.at[k], self.p.sib).wait_recv()

    def over_z(self, k):
        p = self.p
        where = self.piece(p.y, p.core)
        rcopy(self.near.at[k, where], self.far.at[k, where], self.sent, self.cr.at[k], p.cross).start()

    def stage0(self, k):
        p = self.p
        self.arrived(k, 4, self.cr)
        self.move(k, self.piece(p.y, p.core, p.zl, 3), self.y1r, p.yr)
        self.move(k, self.piece(p.y, p.core, p.zl, 3), self.y1r, p.yl)
        self.move(k, self.piece(p.y, p.core), self.dr, p.sib)

    def stage1(self, k):
        p = self.p
        self.arrived(k, 6, self.y1r)
        self.move(k, self.piece(p.ym, p.core, 2 * p.zl, 1), self.y2r, p.yr)
        self.move(k, self.piece(p.yp, p.core, 2 * p.zl + 1, 1), self.y2r, p.yl)
        self.move(k, self.piece(p.ym, p.core, 3 * p.zl, 1), self.z1r, p.zpart)
        self.move(k, self.piece(p.yp, p.core, 3 * p.zl, 1), self.z1r, p.zpart)

    def stage2(self, k):
        p = self.p
        self.arrived(k, 2, self.y2r)
        self.move(k, self.piece(p.yo, p.core, 2 * p.zl, 2), self.z2r, p.zpart)
        self.arrived(k, 2, self.z1r)
        self.move(k, self.piece(p.ym, p.core), self.dr, p.sib)
        self.move(k, self.piece(p.yp, p.core), self.dr, p.sib)

    def stage3(self, k):
        p = self.p
        self.arrived(k, 2, self.z2r)
        self.move(k, self.piece(p.yo, p.core), self.dr, p.sib)

    def ready(self, k):
        self.arrived(k, 16, self.dr)

    def drain(self):
        rcopy(self.far, self.far, self.sent, self.sent, self.p.sib).wait_send()


def kernel(
    gain, head, length, resid_h, wq_h, wkv_h, wo_h, pol_h,
    hid_o, rew_o, pol_o,
    rv, tok, wl, wr, ol, fr, acc, qv, kvs, kva, att, part, r1, r2, hid, racc, rsend, rrecv, pol,
    lsem, wsem, osem, tsent, t1r, t2r,
    asent, acr, ay1r, ay2r, az1r, az2r, adr,
    bsent, bcr, by1r, by2r, bz1r, bz2r, bdr,
    ks, kr, ssent, s1r, s2r, hsem, wsent, wrecv, psent, pr, psem,
):
    p = Place()
    ea = Exchange(p, wl, wr, CW, (asent, acr, ay1r, ay2r, az1r, az2r, adr))
    eb = Exchange(p, ol, fr, QC, (bsent, bcr, by1r, by2r, bz1r, bz2r, bdr))

    barrier = pltpu.get_barrier_semaphore()
    for t in range(8):
        @pl.when(t != p.tp)
        def _():
            pl.semaphore_signal(barrier, inc=1, device_id=(p.rep, t), device_id_type=MESH)
    for dev in (p.yr, p.yl, p.cross, p.zpart, p.sib):
        pl.semaphore_signal(barrier, inc=1, device_id=dev, device_id_type=MESH)

    root = (p.zl == 0) & (p.y == 0) & (p.core == 0)

    for k in range(N):
        pltpu.make_async_copy(resid_h.at[:, pl.ds(k * CW, CW)], rv.at[k], lsem).start()

    @pl.loop(0, N)
    def _(k):
        at = pl.ds(pl.multiple_of(k * CW, CW), CW)
        pltpu.make_async_copy(wq_h.at[at], wl.at[k, :, pl.ds(0, QC)], wsem.at[k]).start()
        pltpu.make_async_copy(wkv_h.at[at], wl.at[k, :, pl.ds(QC, 128)], wsem.at[k]).start()

    @pl.loop(0, N)
    def _(k):
        at = pl.ds(pl.multiple_of(k * CW, CW), CW)
        pltpu.make_async_copy(wo_h.at[:, at], ol.at[k], osem).start()

    load_pol = pltpu.make_async_copy(pol_h, pol, psem)

    @pl.when(root)
    def _():
        load_pol.start()

    own = pl.ds(pl.multiple_of(p.x * ROWS, ROWS), ROWS)
    pltpu.make_async_copy(rv, rv, lsem).wait()
    squares = jnp.zeros((ROWS, 1), F32)
    for k in range(N):
        r = rv[k].astype(F32)
        squares += jnp.sum(r * r, axis=-1, keepdims=True)
    scale = lax.rsqrt(squares / D + 1e-05)
    for k in range(N):
        g = gain[k * CW : (k + 1) * CW].astype(F32).reshape(1, CW)
        tok[k, own, :] = (rv[k].astype(F32) * scale * g).astype(BF)

    pl.semaphore_wait(barrier, 12)

    def block(xx, start=0, size=ROWS):
        return pl.ds(pl.multiple_of(xx * ROWS + start, 16), size)

    def token_move(k, where, rsem, dev):
        ref = tok.at[k, where]
        rcopy(ref, ref, tsent, rsem.at[k], dev).start()

    def token_arrived(k, count, rsem):
        ref = tok.at[k, pl.ds(0, count)]
        rcopy(ref, ref, tsent, rsem.at[k], p.sib).wait_recv()

    def tokens_send(k):
        token_move(k, block(p.x), t1r, p.xr)
        token_move(k, block(p.x), t1r, p.xl)

    def tokens_forward(k):
        token_arrived(k, 2 * ROWS, t1r)
        token_move(k, block(p.xm, 0, 32), t2r, p.xr)
        token_move(k, block(p.xp, 32, 32), t2r, p.xl)

    for k in range(2):
        tokens_send(k)

    @pl.loop(0, N)
    def _(k):
        pltpu.make_async_copy(wl.at[k], wl.at[k], wsem.at[k]).wait()
        ea.over_z(k)

    acc[...] = jnp.zeros_like(acc)

    def project(k):
        token_arrived(k, ROWS, t2r)
        ea.ready(k)
        acc[p.zh] = acc[p.zh] + jnp.dot(tok[k], wl[k], preferred_element_type=F32)
        acc[1 - p.zh] = acc[1 - p.zh] + jnp.dot(tok[k], wr[k], preferred_element_type=F32)

    def step_b(j):
        @pl.when(j == -3)
        def _():
            pltpu.make_async_copy(ol, ol, osem).wait()

        when_in(j + 3, 0, N, eb.over_z)
        when_in(j - 6, 0, N, eb.stage3)
        when_in(j - 5, 0, N, eb.stage2)
        when_in(j - 4, 0, N, eb.stage1)
        when_in(j, 0, N, eb.stage0)

    @pl.loop(0, N + 4)
    def _(i):
        when_in(i + 2, 0, N, tokens_send)
        when_in(i - 1, 0, N, tokens_forward)
        when_in(i - 3, 0, N, ea.stage3)
        when_in(i - 2, 0, N, ea.stage2)
        when_in(i - 1, 0, N, ea.stage1)
        when_in(i, 0, N, ea.stage0)
        step_b(i - N)
        when_in(i - 4, 0, N, project)

    first = (p.zl == 0) & (p.core == 0)
    ups = p.y < 3
    downs = (p.y == 0) | (p.y > 1)
    hops = (p.y, lax.rem(4 - p.y, 4))

    def pol_move(way, m, dev):
        rcopy(pol.at[m], pol.at[m], psent.at[way], pr.at[m], dev).start()

    def pol_arrived(m):
        rcopy(pol.at[m], pol.at[m], psem, pr.at[m], p.sib).wait_recv()

    def pol_fan(m):
        pol_move(2, m, p.zpart)
        pol_move(3, m, p.sib)

    def pol_step(j):
        @pl.when(root & (j == 4))
        def _():
            load_pol.wait()

        for d in (0, 1):
            t = j - 4 - LAG * hops[d]
            m = t // 2

            @pl.when(first & (t >= 0) & (t < 8) & (lax.rem(t, 2) == 0))
            def _():
                @pl.when(p.y > 0)
                def _():
                    pol_arrived(4 * d + m)

                @pl.when(downs if d else ups)
                def _():
                    pol_move(d, 4 * d + m, p.yl if d else p.yr)

                pol_fan(4 * d + m)

            t2 = t - LAG
            m2 = t2 // 2

            @pl.when((p.zl == 1) & (p.core == 0) & (t2 >= 0) & (t2 < 8) & (lax.rem(t2, 2) == 0))
            def _():
                pol_arrived(4 * d + m2)
                pol_move(3, 4 * d + m2, p.sib)

    for kind in (0, 1):
        kvs[kind] = acc[kind, :, QC:].astype(BF)
    slot = p.x // 2
    here = pl.ds(pl.multiple_of(p.zh * PLANE, PLANE), PLANE)
    targets = [(kind, xd, zd) for kind in (0, 1) for zd in (1, 0) for xd in (0, 1)]

    def kv_target(kind, xd, zd):
        to = zd * 4 + 2 * lax.rem(p.x, 2) + xd
        return to, rcopy(
            kvs.at[kind], kva.at[kind, slot, here], ks.at[kind, 2 * zd + xd],
            kr.at[kind, slot * 2 + p.zh], (p.rep, to),
        )

    for target in targets:
        to, copy = kv_target(*target)

        @pl.when((to != p.tp) & (target[2] >= p.zh))
        def _():
            copy.start()

        @pl.when(to == p.tp)
        def _():
            kva[target[0], slot, here, :] = kvs[target[0]]

    for s in (0, 1):
        qv[s] = acc[s, :, :QC].astype(BF)
    step_b(jnp.int32(4))
    pol_step(jnp.int32(4))

    def kv_arrived(kind, planes):
        for j in (0, 1):
            for pz in range(planes):
                @pl.when(pz * 4 + 2 * j + p.x // 2 != p.tp)
                def _():
                    ref = kva.at[kind, j, pl.ds(pz * PLANE, PLANE)]
                    rcopy(ref, ref, ks.at[0, 0], kr.at[kind, j * 2 + pz], p.sib).wait_recv()

    last = length[0]

    def attend(pair, planes):
        keys = planes * PLANE
        rowpos = lax.broadcasted_iota(jnp.int32, (PLANE, keys), 0) + (planes - 1) * PLANE
        colpos = lax.broadcasted_iota(jnp.int32, (PLANE, keys), 1)
        valid = (colpos <= rowpos) & (colpos < last)
        if pair == 0:
            kv_arrived(0, planes)
        for half in (0, 1):
            s, h = pair // 2, 2 * (pair % 2) + half
            cols = slice(h * HS, (h + 1) * HS)
            scores = lax.dot_general(
                qv[s, :, cols], kva[0, s, :keys, :], (((1,), (1,)), ((), ())),
                preferred_element_type=F32,
            )
            scores = jnp.where(valid, scores, -1e30)
            top = jnp.max(scores, axis=-1, keepdims=True)
            weight = jnp.exp2((scores - top) * (HS ** (-0.5) * 1.4426950408889634))
            probs = (weight * (1.0 / jnp.sum(weight, axis=-1, keepdims=True))).astype(BF)
            if pair == 0 and half == 0:
                kv_arrived(1, planes)
            att[s, :, cols] = jnp.dot(probs, kva[1, s, :keys, :], preferred_element_type=F32).astype(BF)

    for pair in range(4):
        for plane in (0, 1):
            @pl.when(p.zh == plane)
            def _():
                attend(pair, plane + 1)
        step_b(jnp.int32(5 + pair))
        pol_step(jnp.int32(5 + pair))

    HALF = CW // 2

    def out_project(c):
        eb.ready(c)
        part[c] = (
            jnp.dot(att[p.zh], ol[c], preferred_element_type=F32)
            + jnp.dot(att[1 - p.zh], fr[c], preferred_element_type=F32)
        ).astype(BF)
        for d, dev in enumerate((p.xr, p.xl)):
            src = part.at[c, block(p.xo), pl.ds(d * HALF, HALF)]
            rcopy(src, r1.at[c, d], ssent, s1r.at[c], dev).start()

    def pass_on(c):
        rcopy(r1.at[c], r1.at[c], ssent, s1r.at[c], p.sib).wait_recv()
        for d, dev in enumerate((p.xr, p.xl)):
            rows, cols = block(p.xm if d else p.xp), pl.ds(d * HALF, HALF)
            part[c, rows, cols] = (part[c, rows, cols].astype(F32) + r1[c, d].astype(F32)).astype(BF)
            rcopy(part.at[c, rows], r2.at[c, d], ssent, s2r.at[c], dev).start()

    def finish(c):
        rcopy(r2.at[c], r2.at[c], ssent, s2r.at[c], p.sib).wait_recv()
        at = pl.ds(pl.multiple_of(c * CW, CW), CW)
        summed = part[c, own, :].astype(F32) + r2[c, 0].astype(F32) + r2[c, 1].astype(F32)
        out = (rv[c].astype(F32) + summed).astype(BF)
        hid[c] = out
        racc[...] = racc[...] + out.astype(F32) * head[at].astype(F32).reshape(1, CW)
        pltpu.make_async_copy(hid.at[c], hid_o.at[:, at], hsem).start()

    racc[...] = jnp.zeros_like(racc)

    @pl.loop(0, max(N + 2, 4 * LAG + 2))
    def _(it):
        step_b(it + 9)
        when_in(it, 0, N, out_project)
        when_in(it - 1, 0, N, pass_on)
        when_in(it - 2, 0, N, finish)
        pol_step(it + 9)

    @pl.when(p.core == 1)
    def _():
        for m in range(PCH):
            pol_arrived(m)

    store_pol = pltpu.make_async_copy(pol, pol_o, psem)
    store_pol.start()

    rows = jnp.sum(racc[...], axis=-1, keepdims=True)
    position = lax.broadcasted_iota(jnp.int32, (ROWS, 1), 0) + p.tp * ROWS
    picked = jnp.where(position == last - 1, 1.0, 0.0) + 512 ** (-0.5)
    share = jnp.sum(rows * picked, axis=0, keepdims=True)
    rsend[...] = jnp.broadcast_to(share, (8, 128))

    for t in range(8):
        @pl.when(t != p.tp)
        def _():
            rcopy(rsend, rrecv.at[p.tp], wsent, wrecv, (p.rep, t)).start()

        @pl.when(t == p.tp)
        def _():
            rrecv[t] = rsend[...]

    ea.drain()
    eb.drain()
    sent = tok.at[:, pl.ds(0, 3 * ROWS)]
    rcopy(sent, sent, tsent, tsent, p.sib).wait_send()
    sent = part.at[:, pl.ds(0, 3 * ROWS)]
    rcopy(sent, sent, ssent, ssent, p.sib).wait_send()
    pltpu.make_async_copy(hid, hid, hsem).wait()

    for target in targets:
        to, copy = kv_target(*target)

        @pl.when((to != p.tp) & (target[2] >= p.zh))
        def _():
            copy.wait_send()

    def pol_sent(way, start, size):
        ref = pol.at[pl.ds(start, size)]
        rcopy(ref, ref, psent.at[way], psem, p.sib).wait_send()

    @pl.when(first & ups)
    def _():
        pol_sent(0, 0, 4)

    @pl.when(first & downs)
    def _():
        pol_sent(1, 4, 4)

    @pl.when(first)
    def _():
        pol_sent(2, 0, PCH)

    @pl.when(p.core == 0)
    def _():
        pol_sent(3, 0, PCH)

    sent = rrecv.at[pl.ds(0, 7)]
    rcopy(sent, sent, wsent, wrecv, p.sib).wait()
    rew_o[0] = jnp.max(jnp.sum(rrecv[...], axis=0))
    store_pol.wait()


def on_device(residual_in, norm_gain, w_query, w_keyval, w_out, score_head, lengths, policy_slots):
    vmem = pl.BlockSpec(memory_space=pltpu.VMEM)
    smem = pl.BlockSpec(memory_space=pltpu.SMEM)
    hbm = pl.BlockSpec(memory_space=pl.ANY)
    dma = pltpu.SemaphoreType.DMA

    exchange_sems = [dma] + [dma((N,))] * 6
    prow = policy_slots.shape[1]
    hidden, reward, policy = pl.pallas_call(
        kernel,
        out_shape=(
            jax.ShapeDtypeStruct((ROWS, D), BF),
            jax.ShapeDtypeStruct((1,), F32),
            jax.ShapeDtypeStruct((PCH, prow // PCH, 1024), BF),
        ),
        in_specs=[vmem, vmem, smem, hbm, hbm, hbm, hbm, hbm],
        out_specs=(hbm, smem, hbm),
        scratch_shapes=[
            pltpu.VMEM((N, ROWS, CW), BF),
            pltpu.VMEM((N, PLANE, CW), BF),
            pltpu.VMEM((N, CW, WC), BF),
            pltpu.VMEM((N, CW, WC), BF),
            pltpu.VMEM((N, 512, CW), BF),
            pltpu.VMEM((N, 512, CW), BF),
            pltpu.VMEM((2, PLANE, WC), F32),
            pltpu.VMEM((2, PLANE, QC), BF),
            pltpu.VMEM((2, PLANE, HS), BF),
            pltpu.VMEM((2, 2, 2 * PLANE, HS), BF),
            pltpu.VMEM((2, PLANE, QC), BF),
            pltpu.VMEM((N, PLANE, CW), BF),
            pltpu.VMEM((N, 2, ROWS, CW // 2), BF),
            pltpu.VMEM((N, 2, ROWS, CW), BF),
            pltpu.VMEM((N, ROWS, CW), BF),
            pltpu.VMEM((ROWS, CW), F32),
            pltpu.VMEM((8, 128), F32),
            pltpu.VMEM((8, 8, 128), F32),
            pltpu.VMEM((PCH, prow // PCH, 1024), BF),
            dma, dma((N,)), dma, dma, dma((N,)), dma((N,)),
            *exchange_sems,
            *exchange_sems,
            dma((2, 4)), dma((2, 4)), dma, dma((N,)), dma((N,)),
            dma, dma, dma, dma((4,)), dma((PCH,)), dma,
        ],
        compiler_params=pltpu.CompilerParams(
            collective_id=0, has_side_effects=True, vmem_limit_bytes=66_000_000
        ),
        name="block",
    )(
        norm_gain, score_head, lengths,
        residual_in[0], w_query, w_keyval, w_out, policy_slots[0].reshape(PCH, prow // PCH, 1024),
    )
    return hidden[None], reward, policy.reshape(1, prow, 1024)


def solution(mesh):
    placed = (
        P("rep", "tp", None),
        P(),
        P(None, "tp"),
        P(None, "tp"),
        P("tp", None),
        P(),
        P("rep"),
        P("rep", None, "tp"),
    )
    return jax.shard_map(
        on_device,
        mesh=mesh,
        in_specs=placed,
        out_specs=(P("rep", "tp", None), P("rep"), P("rep", None, "tp")),
        check_vma=False,
    )
```

```python
import functools

import jax
import jax.numpy as jnp
from jax import lax
from jax.experimental import pallas as pl
from jax.experimental.pallas import tpu as pltpu
from jax.sharding import PartitionSpec as P

HS = 128
N = 16
D = 8192
CW = D // N
ROWS = 64
PLANE = 256
QC = 512
KC = 128
PCH = 16
NK = 4
E1, E2, E3, EP = 3, 6, 9, 11
KV0, Q0, O0 = 0, NK, NK + N
STEPS = O0 + N
AHEAD = 4
GAP = O0 + EP
RL = 3
POL = GAP + 1
LAG = 2
WG = 4
MESH = pl.DeviceIdType.MESH
BF = jnp.bfloat16
F32 = jnp.float32


def rcopy(src, dst, ssem, rsem, dev):
    return pltpu.make_async_remote_copy(
        src_ref=src, dst_ref=dst, send_sem=ssem, recv_sem=rsem, device_id=dev, device_id_type=MESH
    )


def when_in(value, low, high, fn):
    @pl.when((value >= low) & (value < high))
    def _():
        fn(value)


class Place:
    def __init__(self):
        rep = lax.axis_index("rep")
        tp = lax.axis_index("tp")
        self.rep, self.tp = rep, tp
        self.core = core = lax.rem(rep, 2)
        self.y = y = lax.rem(rep // 2, 4)
        self.zl = zl = rep // 8
        self.x = x = lax.rem(tp, 4)
        self.zh = zh = tp // 4
        self.xp, self.xm, self.xo = lax.rem(x + 1, 4), lax.rem(x + 3, 4), lax.rem(x + 2, 4)
        self.yp, self.ym, self.yo = lax.rem(y + 1, 4), lax.rem(y + 3, 4), lax.rem(y + 2, 4)
        self.xr = (rep, zh * 4 + self.xp)
        self.xl = (rep, zh * 4 + self.xm)
        self.yr = ((zl * 4 + self.yp) * 2 + core, tp)
        self.yl = ((zl * 4 + self.ym) * 2 + core, tp)
        self.cross = (((1 - zl) * 4 + y) * 2 + core, (1 - zh) * 4 + x)
        self.zpart = (((1 - zl) * 4 + y) * 2 + core, tp)
        self.sib = (rep + 1 - 2 * core, tp)


class Exchange:
    def __init__(self, p, near, far, base, sems):
        self.p, self.near, self.far, self.base = p, near, far, base
        self.count, self.rows = far.shape[:2]
        self.sent, self.cr, self.y1r, self.y2r, self.z2r, self.dr = sems

    def piece(self, yy, core, sub=0, subs=4):
        size = self.rows // 32
        start = yy * (self.rows // 4) + core * (self.rows // 8) + sub * size
        return pl.ds(pl.multiple_of(start, 16), subs * size)

    def move(self, k, where, rsem, dev):
        ref = self.far.at[k, where]
        rcopy(ref, ref, self.sent, rsem.at[self.base + k], dev).start()

    def arrived(self, k, count, rsem):
        ref = self.far.at[k, pl.ds(0, count * (self.rows // 32))]
        rcopy(ref, ref, self.sent, rsem.at[self.base + k], self.p.sib).wait_recv()

    def over_z(self, k):
        p = self.p
        where = self.piece(p.y, p.core)
        rcopy(
            self.near.at[k, where], self.far.at[k, where], self.sent, self.cr.at[self.base + k], p.cross
        ).start()

    def stage0(self, k):
        p = self.p
        self.arrived(k, 4, self.cr)
        self.move(k, self.piece(p.y, p.core, p.zl, 3), self.y1r, p.yr)
        self.move(k, self.piece(p.y, p.core, p.zl, 3), self.y1r, p.yl)
        self.move(k, self.piece(p.y, p.core), self.dr, p.sib)

    def stage1(self, k):
        p = self.p
        self.arrived(k, 6, self.y1r)
        self.move(k, self.piece(p.ym, p.core, 2 * p.zl, 1), self.y2r, p.yr)
        self.move(k, self.piece(p.yp, p.core, 2 * p.zl + 1, 1), self.y2r, p.yl)
        self.move(k, self.piece(p.ym, p.core, 3 * p.zl, 1), self.y2r, p.zpart)
        self.move(k, self.piece(p.yp, p.core, 3 * p.zl, 1), self.y2r, p.zpart)

    def stage2(self, k):
        p = self.p
        self.arrived(k, 4, self.y2r)
        self.move(k, self.piece(p.yo, p.core, 2 * p.zl, 2), self.z2r, p.zpart)
        self.move(k, self.piece(p.ym, p.core), self.dr, p.sib)
        self.move(k, self.piece(p.yp, p.core), self.dr, p.sib)

    def stage3(self, k):
        p = self.p
        self.arrived(k, 2, self.z2r)
        self.move(k, self.piece(p.yo, p.core), self.dr, p.sib)

    def ready(self, k):
        self.arrived(k, 16, self.dr)

    def stages(self, i):
        k = i - self.base
        when_in(k - E3, 0, self.count, self.stage3)
        when_in(k - E2, 0, self.count, self.stage2)
        when_in(k - E1, 0, self.count, self.stage1)
        when_in(k, 0, self.count, self.stage0)

    def drain(self):
        rcopy(self.far, self.far, self.sent, self.sent, self.p.sib).wait_send()


def kernel(
    gain, head, length, resid_h, wq_h, wkv_h, wo_h, pol_h,
    hid_o, rew_o, pol_o,
    rv, tok, wkl, wkr, wql, wqr, wol, wor, kacc, qacc, qv, kvs, kva, att, part, r1, r2, hid, racc, rsend, rrecv, pol,
    lsem, wksem, wqsem, wosem, tsent, t1r, t2r,
    ksent, qsent, osent, cr, y1r, y2r, z2r, dr,
    ks, kr, ssent, s1r, s2r, hsem, wsent, wrecv, psent, pr, psem,
):
    p = Place()
    recvs = (cr, y1r, y2r, z2r, dr)
    ek = Exchange(p, wkl, wkr, KV0, (ksent, *recvs))
    eq = Exchange(p, wql, wqr, Q0, (qsent, *recvs))
    eo = Exchange(p, wol, wor, O0, (osent, *recvs))

    barrier = pltpu.get_barrier_semaphore()
    for t in range(8):
        @pl.when(t != p.tp)
        def _():
            pl.semaphore_signal(barrier, inc=1, device_id=(p.rep, t), device_id_type=MESH)
    for dev in (p.yr, p.yl, p.cross, p.zpart, p.sib):
        pl.semaphore_signal(barrier, inc=1, device_id=dev, device_id_type=MESH)

    root = (p.zl == 0) & (p.y == 0) & (p.core == 0)

    for k in range(N):
        pltpu.make_async_copy(resid_h.at[:, pl.ds(k * CW, CW)], rv.at[k], lsem).start()

    load_wk = pltpu.make_async_copy(wkv_h, wkl, wksem)
    load_wk.start()
    for g in range(WG):
        part_of = pl.ds(g * N // WG, N // WG)
        pltpu.make_async_copy(wq_h.at[part_of], wql.at[part_of], wqsem.at[g]).start()

    @pl.loop(0, N)
    def _(k):
        at = pl.ds(pl.multiple_of(k * CW, CW), CW)
        pltpu.make_async_copy(wo_h.at[:, at], wol.at[k], wosem).start()

    load_pol = pltpu.make_async_copy(pol_h, pol, psem)

    @pl.when(root)
    def _():
        load_pol.start()

    own = pl.ds(pl.multiple_of(p.x * ROWS, ROWS), ROWS)
    pltpu.make_async_copy(rv, rv, lsem).wait()
    squares = jnp.zeros((ROWS, 1), F32)
    for k in range(N):
        r = rv[k].astype(F32)
        squares += jnp.sum(r * r, axis=-1, keepdims=True)
    scale = lax.rsqrt(squares / D + 1e-05)
    for k in range(N):
        g = gain[k * CW : (k + 1) * CW].astype(F32).reshape(1, CW)
        tok[k, own, :] = (rv[k].astype(F32) * scale * g).astype(BF)

    pl.semaphore_wait(barrier, 12)

    def block(xx, start=0, size=ROWS):
        return pl.ds(pl.multiple_of(xx * ROWS + start, 16), size)

    def token_move(k, where, rsem, dev):
        ref = tok.at[k, where]
        rcopy(ref, ref, tsent, rsem.at[k], dev).start()

    def token_arrived(k, count, rsem):
        ref = tok.at[k, pl.ds(0, count)]
        rcopy(ref, ref, tsent, rsem.at[k], p.sib).wait_recv()

    def tokens_send(k):
        token_move(k, block(p.x), t1r, p.xr)
        token_move(k, block(p.x), t1r, p.xl)

    def tokens_forward(k):
        token_arrived(k, 2 * ROWS, t1r)
        token_move(k, block(p.xm, 0, 32), t2r, p.xr)
        token_move(k, block(p.xp, 32, 32), t2r, p.xl)

    for k in range(2):
        tokens_send(k)

    load_wk.wait()
    for k in range(NK):
        ek.over_z(k)
    for g in range(WG):
        part_of = pl.ds(g * N // WG, N // WG)
        pltpu.make_async_copy(wq_h.at[part_of], wql.at[part_of], wqsem.at[g]).wait()

        @pl.loop(g * N // WG, (g + 1) * N // WG)
        def _(k):
            eq.over_z(k)

    kacc[...] = jnp.zeros_like(kacc)
    qacc[...] = jnp.zeros_like(qacc)

    def project_kv(k):
        token_arrived(k, ROWS, t2r)

        @pl.when(lax.rem(k, N // NK) == 0)
        def _():
            ek.ready(k // (N // NK))

        rows = pl.ds(pl.multiple_of(lax.rem(k, N // NK) * CW, CW), CW)
        for shard, w in ((p.zh, wkl), (1 - p.zh, wkr)):
            kacc[shard] = kacc[shard] + jnp.dot(
                tok[k], w[k // (N // NK), rows, :], preferred_element_type=F32
            )

    def project_q(k):
        eq.ready(k)
        qacc[p.zh] = qacc[p.zh] + jnp.dot(tok[k], wql[k], preferred_element_type=F32)
        qacc[1 - p.zh] = qacc[1 - p.zh] + jnp.dot(tok[k], wqr[k], preferred_element_type=F32)

    def step(i):
        @pl.when(i == O0 - AHEAD)
        def _():
            pltpu.make_async_copy(wol, wol, wosem).wait()

        when_in(i - O0 + AHEAD, 0, N, eo.over_z)
        for exchange in (ek, eq, eo):
            exchange.stages(i)

    def token_step(c):
        when_in(c + 2, 0, N, tokens_send)
        when_in(c, 0, N, tokens_forward)

    first = (p.zl == 0) & (p.core == 0)
    ups = p.y < 3
    downs = (p.y == 0) | (p.y > 1)
    hops = (p.y, lax.rem(4 - p.y, 4))

    def pol_move(way, m, dev):
        rcopy(pol.at[m], pol.at[m], psent.at[way], pr.at[m], dev).start()

    def pol_arrived(m):
        rcopy(pol.at[m], pol.at[m], psem, pr.at[m], p.sib).wait_recv()

    def pol_step(j):
        @pl.when(root & (j == POL))
        def _():
            load_pol.wait()

        for d in (0, 1):
            t = j - POL - LAG * hops[d]
            m = PCH // 2 * d + t // 2

            @pl.when(first & (t >= 0) & (t < PCH) & (lax.rem(t, 2) == d))
            def _():
                @pl.when(p.y > 0)
                def _():
                    pol_arrived(m)

                @pl.when(downs if d else ups)
                def _():
                    pol_move(d, m, p.yl if d else p.yr)

                pol_move(2, m, p.zpart)
                pol_move(3, m, p.sib)

            t2 = t - LAG
            m2 = PCH // 2 * d + t2 // 2

            @pl.when((p.zl == 1) & (p.core == 0) & (t2 >= 0) & (t2 < PCH) & (lax.rem(t2, 2) == d))
            def _():
                pol_arrived(m2)
                pol_move(3, m2, p.sib)

    slot = p.x // 2
    here = pl.ds(pl.multiple_of(p.zh * PLANE, PLANE), PLANE)
    targets = [(kind, xd, zd) for kind in (0, 1) for zd in (0, 1) for xd in (0, 1)]

    def kv_target(kind, xd, zd):
        to = zd * 4 + 2 * lax.rem(p.x, 2) + xd
        return to, rcopy(
            kvs.at[kind], kva.at[kind, slot, here], ks.at[kind, 2 * zd + xd],
            kr.at[kind, slot * 2 + p.zh], (p.rep, to),
        )

    def kv_send():
        for kind in (0, 1):
            kvs[kind] = kacc[kind].astype(BF)
        for target in targets:
            to, copy = kv_target(*target)

            @pl.when((to != p.tp) & (target[2] >= p.zh))
            def _():
                copy.start()

            @pl.when(to == p.tp)
            def _():
                kva[target[0], slot, here, :] = kvs[target[0]]

    @pl.loop(0, GAP)
    def _(i):
        c, off = 2 * i // 3, lax.rem(2 * i, 3)

        @pl.when(off != 2)
        def _():
            token_step(c)

        step(i)

        when_in(i - EP - 1, 0, N, project_kv)

        @pl.when(i == EP + N)
        def _():
            kv_send()

        when_in(i - Q0 - EP, 0, N, project_q)

    for s in (0, 1):
        qv[s] = qacc[s].astype(BF)
    step(jnp.int32(GAP))

    def kv_arrived(kind, planes):
        for j in (0, 1):
            for pz in range(planes):
                @pl.when(pz * 4 + 2 * j + p.x // 2 != p.tp)
                def _():
                    ref = kva.at[kind, j, pl.ds(pz * PLANE, PLANE)]
                    rcopy(ref, ref, ks.at[0, 0], kr.at[kind, j * 2 + pz], p.sib).wait_recv()

    last = length[0]

    def attend(pair, planes):
        keys = planes * PLANE
        rowpos = lax.broadcasted_iota(jnp.int32, (PLANE, keys), 0) + (planes - 1) * PLANE
        colpos = lax.broadcasted_iota(jnp.int32, (PLANE, keys), 1)
        valid = (colpos <= rowpos) & (colpos < last)
        if pair == 0:
            kv_arrived(0, planes)
        for half in (0, 1):
            s, h = pair // 2, 2 * (pair % 2) + half
            cols = slice(h * HS, (h + 1) * HS)
            scores = lax.dot_general(
                qv[s, :, cols], kva[0, s, :keys, :], (((1,), (1,)), ((), ())),
                preferred_element_type=F32,
            )
            scores = jnp.where(valid, scores, -1e30)
            top = jnp.max(scores, axis=-1, keepdims=True)
            weight = jnp.exp2((scores - top) * (HS ** (-0.5) * 1.4426950408889634))
            probs = (weight * (1.0 / jnp.sum(weight, axis=-1, keepdims=True))).astype(BF)
            if pair == 0 and half == 0:
                kv_arrived(1, planes)
            att[s, :, cols] = jnp.dot(probs, kva[1, s, :keys, :], preferred_element_type=F32).astype(BF)

    for pair in range(4):
        for plane in (0, 1):
            @pl.when(p.zh == plane)
            def _():
                attend(pair, plane + 1)
        step(jnp.int32(GAP + 1 + pair))
        pol_step(jnp.int32(GAP + 1 + pair))

    HALF = CW // 2

    def out_project(c):
        eo.ready(c)
        part[c] = (
            jnp.dot(att[p.zh], wol[c], preferred_element_type=F32)
            + jnp.dot(att[1 - p.zh], wor[c], preferred_element_type=F32)
        ).astype(BF)
        for d, dev in enumerate((p.xr, p.xl)):
            src = part.at[c, block(p.xo), pl.ds(d * HALF, HALF)]
            rcopy(src, r1.at[c, d], ssent, s1r.at[c], dev).start()

    def pass_on(c):
        rcopy(r1.at[c], r1.at[c], ssent, s1r.at[c], p.sib).wait_recv()
        for d, dev in enumerate((p.xr, p.xl)):
            rows, cols = block(p.xm if d else p.xp), pl.ds(d * HALF, HALF)
            part[c, rows, cols] = (part[c, rows, cols].astype(F32) + r1[c, d].astype(F32)).astype(BF)
            rcopy(part.at[c, rows], r2.at[c, d], ssent, s2r.at[c], dev).start()

    def finish(c):
        rcopy(r2.at[c], r2.at[c], ssent, s2r.at[c], p.sib).wait_recv()
        at = pl.ds(pl.multiple_of(c * CW, CW), CW)
        summed = part[c, own, :].astype(F32) + r2[c, 0].astype(F32) + r2[c, 1].astype(F32)
        out = (rv[c].astype(F32) + summed).astype(BF)
        hid[c] = out
        racc[...] = racc[...] + out.astype(F32) * head[at].astype(F32).reshape(1, CW)
        pltpu.make_async_copy(hid.at[c], hid_o.at[:, at], hsem).start()

    racc[...] = jnp.zeros_like(racc)

    @pl.loop(0, max(N + 2 * RL, PCH + 4 * LAG - 4))
    def _(it):
        when_in(it - RL, 0, N, pass_on)
        step(it + GAP + 5)
        when_in(it, 0, N, out_project)
        when_in(it - 2 * RL, 0, N, finish)
        pol_step(it + GAP + 5)

    @pl.when(p.core == 1)
    def _():
        for m in range(PCH):
            pol_arrived(m)

    store_pol = pltpu.make_async_copy(pol, pol_o, psem)
    store_pol.start()

    rows = jnp.sum(racc[...], axis=-1, keepdims=True)
    position = lax.broadcasted_iota(jnp.int32, (ROWS, 1), 0) + p.tp * ROWS
    picked = jnp.where(position == last - 1, 1.0, 0.0) + 512 ** (-0.5)
    share = jnp.sum(rows * picked, axis=0, keepdims=True)
    rsend[...] = jnp.broadcast_to(share, (8, 128))

    for t in range(8):
        @pl.when(t != p.tp)
        def _():
            rcopy(rsend, rrecv.at[p.tp], wsent, wrecv, (p.rep, t)).start()

        @pl.when(t == p.tp)
        def _():
            rrecv[t] = rsend[...]

    for exchange in (ek, eq, eo):
        exchange.drain()
    sent = tok.at[:, pl.ds(0, 3 * ROWS)]
    rcopy(sent, sent, tsent, tsent, p.sib).wait_send()
    sent = part.at[:, pl.ds(0, 3 * ROWS)]
    rcopy(sent, sent, ssent, ssent, p.sib).wait_send()
    pltpu.make_async_copy(hid, hid, hsem).wait()

    for target in targets:
        to, copy = kv_target(*target)

        @pl.when((to != p.tp) & (target[2] >= p.zh))
        def _():
            copy.wait_send()

    def pol_sent(way, start, size):
        ref = pol.at[pl.ds(start, size)]
        rcopy(ref, ref, psent.at[way], psem, p.sib).wait_send()

    @pl.when(first & ups)
    def _():
        pol_sent(0, 0, PCH // 2)

    @pl.when(first & downs)
    def _():
        pol_sent(1, PCH // 2, PCH // 2)

    @pl.when(first)
    def _():
        pol_sent(2, 0, PCH)

    @pl.when(p.core == 0)
    def _():
        pol_sent(3, 0, PCH)

    sent = rrecv.at[pl.ds(0, 7)]
    rcopy(sent, sent, wsent, wrecv, p.sib).wait()
    rew_o[0] = jnp.max(jnp.sum(rrecv[...], axis=0))
    store_pol.wait()


def on_device(residual_in, norm_gain, w_query, w_keyval, w_out, score_head, lengths, policy_slots):
    vmem = pl.BlockSpec(memory_space=pltpu.VMEM)
    smem = pl.BlockSpec(memory_space=pltpu.SMEM)
    hbm = pl.BlockSpec(memory_space=pl.ANY)
    dma = pltpu.SemaphoreType.DMA

    prow = policy_slots.shape[1]
    hidden, reward, policy = pl.pallas_call(
        kernel,
        out_shape=(
            jax.ShapeDtypeStruct((ROWS, D), BF),
            jax.ShapeDtypeStruct((1,), F32),
            jax.ShapeDtypeStruct((PCH, prow // PCH, 1024), BF),
        ),
        in_specs=[vmem, vmem, smem, hbm, hbm, hbm, hbm, hbm],
        out_specs=(hbm, smem, hbm),
        scratch_shapes=[
            pltpu.VMEM((N, ROWS, CW), BF),
            pltpu.VMEM((N, PLANE, CW), BF),
            pltpu.VMEM((NK, D // NK, KC), BF),
            pltpu.VMEM((NK, D // NK, KC), BF),
            pltpu.VMEM((N, CW, QC), BF),
            pltpu.VMEM((N, CW, QC), BF),
            pltpu.VMEM((N, QC, CW), BF),
            pltpu.VMEM((N, QC, CW), BF),
            pltpu.VMEM((2, PLANE, KC), F32),
            pltpu.VMEM((2, PLANE, QC), F32),
            pltpu.VMEM((2, PLANE, QC), BF),
            pltpu.VMEM((2, PLANE, HS), BF),
            pltpu.VMEM((2, 2, 2 * PLANE, HS), BF),
            pltpu.VMEM((2, PLANE, QC), BF),
            pltpu.VMEM((N, PLANE, CW), BF),
            pltpu.VMEM((N, 2, ROWS, CW // 2), BF),
            pltpu.VMEM((N, 2, ROWS, CW), BF),
            pltpu.VMEM((N, ROWS, CW), BF),
            pltpu.VMEM((ROWS, CW), F32),
            pltpu.VMEM((8, 128), F32),
            pltpu.VMEM((8, 8, 128), F32),
            pltpu.VMEM((PCH, prow // PCH, 1024), BF),
            dma, dma, dma((WG,)), dma, dma, dma((N,)), dma((N,)),
            dma, dma, dma, *[dma((STEPS,))] * 5,
            dma((2, 4)), dma((2, 4)), dma, dma((N,)), dma((N,)),
            dma, dma, dma, dma((4,)), dma((PCH,)), dma,
        ],
        compiler_params=pltpu.CompilerParams(
            collective_id=0, has_side_effects=True, vmem_limit_bytes=66_000_000
        ),
        name="block",
    )(
        norm_gain, score_head, lengths,
        residual_in[0], w_query.reshape(N, CW, QC), w_keyval.reshape(NK, D // NK, KC), w_out,
        policy_slots[0].reshape(PCH, prow // PCH, 1024),
    )
    return hidden[None], reward, policy.reshape(1, prow, 1024)


def solution(mesh):
    placed = (
        P("rep", "tp", None),
        P(),
        P(None, "tp"),
        P(None, "tp"),
        P("tp", None),
        P(),
        P("rep"),
        P("rep", None, "tp"),
    )
    return jax.shard_map(
        on_device,
        mesh=mesh,
        in_specs=placed,
        out_specs=(P("rep", "tp", None), P("rep"), P("rep", None, "tp")),
        check_vma=False,
    )
```

```python
import functools

import jax
import jax.numpy as jnp
from jax import lax
from jax.experimental import pallas as pl
from jax.experimental.pallas import tpu as pltpu
from jax.sharding import PartitionSpec as P

HS = 128
N = 16
D = 8192
CW = D // N
ROWS = 64
PLANE = 256
QC = 512
KC = 128
PCH = 16
NK = 4
E1, E2, E3, EP = 3, 6, 9, 10
KV0, Q0, O0 = 0, NK, NK + N
AHEAD = 4
GAP = NK + N + EP
SLOW = 1
V0 = -(-(GAP - O0) // SLOW)
LEAD = 3
RL = 3
POL = 5
LAG = 2
WG = 4
MESH = pl.DeviceIdType.MESH
BF = jnp.bfloat16
F32 = jnp.float32


def rcopy(src, dst, ssem, rsem, dev):
    return pltpu.make_async_remote_copy(
        src_ref=src, dst_ref=dst, send_sem=ssem, recv_sem=rsem, device_id=dev, device_id_type=MESH
    )


def when_in(value, low, high, fn):
    @pl.when((value >= low) & (value < high))
    def _():
        fn(value)


class Place:
    def __init__(self):
        rep = lax.axis_index("rep")
        tp = lax.axis_index("tp")
        self.rep, self.tp = rep, tp
        self.core = core = lax.rem(rep, 2)
        self.y = y = lax.rem(rep // 2, 4)
        self.zl = zl = rep // 8
        self.x = x = lax.rem(tp, 4)
        self.zh = zh = tp // 4
        self.xp, self.xm, self.xo = lax.rem(x + 1, 4), lax.rem(x + 3, 4), lax.rem(x + 2, 4)
        self.yp, self.ym, self.yo = lax.rem(y + 1, 4), lax.rem(y + 3, 4), lax.rem(y + 2, 4)
        self.xr = (rep, zh * 4 + self.xp)
        self.xl = (rep, zh * 4 + self.xm)
        self.yr = ((zl * 4 + self.yp) * 2 + core, tp)
        self.yl = ((zl * 4 + self.ym) * 2 + core, tp)
        self.cross = (((1 - zl) * 4 + y) * 2 + core, (1 - zh) * 4 + x)
        self.zpart = (((1 - zl) * 4 + y) * 2 + core, tp)
        self.sib = (rep + 1 - 2 * core, tp)


class Exchange:
    def __init__(self, p, near, far, first, base, sems):
        self.p, self.near, self.far, self.first, self.base = p, near, far, first, base
        self.count, self.rows = far.shape[:2]
        self.sent, self.cr, self.y1r, self.y2r, self.z2r, self.dr = sems

    def piece(self, yy, core, sub=0, subs=4):
        size = self.rows // 32
        start = yy * (self.rows // 4) + core * (self.rows // 8) + sub * size
        return pl.ds(pl.multiple_of(start, 16), subs * size)

    def move(self, k, where, rsem, dev):
        ref = self.far.at[k, where]
        rcopy(ref, ref, self.sent, rsem.at[self.base + k], dev).start()

    def arrived(self, k, count, rsem):
        ref = self.far.at[k, pl.ds(0, count * (self.rows // 32))]
        rcopy(ref, ref, self.sent, rsem.at[self.base + k], self.p.sib).wait_recv()

    def over_z(self, k):
        p = self.p
        where = self.piece(p.y, p.core)
        rcopy(
            self.near.at[k, where], self.far.at[k, where], self.sent, self.cr.at[self.base + k], p.cross
        ).start()

    def stage0(self, k):
        p = self.p
        self.arrived(k, 4, self.cr)
        self.move(k, self.piece(p.y, p.core, p.zl, 3), self.y1r, p.yr)
        self.move(k, self.piece(p.y, p.core, p.zl, 3), self.y1r, p.yl)
        self.move(k, self.piece(p.y, p.core), self.dr, p.sib)

    def stage1(self, k):
        p = self.p
        self.arrived(k, 6, self.y1r)
        self.move(k, self.piece(p.ym, p.core, 2 * p.zl, 1), self.y2r, p.yr)
        self.move(k, self.piece(p.yp, p.core, 2 * p.zl + 1, 1), self.y2r, p.yl)
        self.move(k, self.piece(p.ym, p.core, 3 * p.zl, 1), self.y2r, p.zpart)
        self.move(k, self.piece(p.yp, p.core, 3 * p.zl, 1), self.y2r, p.zpart)

    def stage2(self, k):
        p = self.p
        self.arrived(k, 4, self.y2r)
        self.move(k, self.piece(p.yo, p.core, 2 * p.zl, 2), self.z2r, p.zpart)
        self.move(k, self.piece(p.ym, p.core), self.dr, p.sib)
        self.move(k, self.piece(p.yp, p.core), self.dr, p.sib)

    def stage3(self, k):
        p = self.p
        self.arrived(k, 2, self.z2r)
        self.move(k, self.piece(p.yo, p.core), self.dr, p.sib)

    def ready(self, k):
        self.arrived(k, 16, self.dr)

    def stages(self, i):
        k = i - self.first
        when_in(k - E3, 0, self.count, self.stage3)
        when_in(k - E2, 0, self.count, self.stage2)
        when_in(k - E1, 0, self.count, self.stage1)
        when_in(k, 0, self.count, self.stage0)

    def drain(self):
        rcopy(self.far, self.far, self.sent, self.sent, self.p.sib).wait_send()


def kernel(
    gain, head, length, resid_h, wq_h, wkv_h, wo_h, pol_h,
    hid_o, rew_o, pol_o,
    rv, tok, wkl, wkr, wql, wqr, wol, wor, kacc, qacc, qv, kvs, kva, att, part, r1, r2, hid, racc, rsend, rrecv, pol,
    lsem, wksem, wqsem, wosem, tsent, t1r, t2r,
    ksent, qsent, osent, cr, y1r, y2r, z2r, dr,
    ks, kr, ssent, s1r, s2r, hsem, wsent, wrecv, psent, pr, psem,
):
    p = Place()
    recvs = (cr, y1r, y2r, z2r, dr)
    ek = Exchange(p, wkl, wkr, KV0, 0, (ksent, *recvs))
    eq = Exchange(p, wql, wqr, Q0, NK, (qsent, *recvs))
    eo = Exchange(p, wol, wor, 0, NK + N, (osent, *recvs))

    barrier = pltpu.get_barrier_semaphore()
    for t in range(8):
        @pl.when(t != p.tp)
        def _():
            pl.semaphore_signal(barrier, inc=1, device_id=(p.rep, t), device_id_type=MESH)
    for dev in (p.yr, p.yl, p.cross, p.zpart, p.sib):
        pl.semaphore_signal(barrier, inc=1, device_id=dev, device_id_type=MESH)

    root = (p.zl == 0) & (p.y == 0) & (p.core == 0)

    for k in range(N):
        pltpu.make_async_copy(resid_h.at[:, pl.ds(k * CW, CW)], rv.at[k], lsem).start()

    load_wk = pltpu.make_async_copy(wkv_h, wkl, wksem)
    load_wk.start()
    own = pl.ds(pl.multiple_of(p.x * ROWS, ROWS), ROWS)
    pltpu.make_async_copy(rv, rv, lsem).wait()
    for g in range(WG):
        part_of = pl.ds(g * N // WG, N // WG)
        pltpu.make_async_copy(wq_h.at[part_of], wql.at[part_of], wqsem.at[g]).start()

    @pl.loop(0, N)
    def _(k):
        at = pl.ds(pl.multiple_of(k * CW, CW), CW)
        pltpu.make_async_copy(wo_h.at[:, at], wol.at[k], wosem).start()

    load_pol = pltpu.make_async_copy(pol_h, pol, psem)

    @pl.when(root)
    def _():
        load_pol.start()

    squares = jnp.zeros((ROWS, 1), F32)
    for k in range(N):
        r = rv[k].astype(F32)
        squares += jnp.sum(r * r, axis=-1, keepdims=True)
    scale = lax.rsqrt(squares / D + 1e-05)
    for k in range(N):
        g = gain[k * CW : (k + 1) * CW].astype(F32).reshape(1, CW)
        tok[k, own, :] = (rv[k].astype(F32) * scale * g).astype(BF)

    pl.semaphore_wait(barrier, 12)

    def block(xx, start=0, size=ROWS):
        return pl.ds(pl.multiple_of(xx * ROWS + start, 16), size)

    def token_move(k, where, rsem, dev):
        ref = tok.at[k, where]
        rcopy(ref, ref, tsent, rsem.at[k], dev).start()

    def token_arrived(k, count, rsem):
        ref = tok.at[k, pl.ds(0, count)]
        rcopy(ref, ref, tsent, rsem.at[k], p.sib).wait_recv()

    def tokens_send(k):
        token_move(k, block(p.x), t1r, p.xr)
        token_move(k, block(p.x), t1r, p.xl)

    def tokens_forward(k):
        token_arrived(k, 2 * ROWS, t1r)
        token_move(k, block(p.xm, 0, 32), t2r, p.xr)
        token_move(k, block(p.xp, 32, 32), t2r, p.xl)

    for k in range(LEAD):
        tokens_send(k)

    load_wk.wait()
    for k in range(NK):
        ek.over_z(k)
    for g in range(WG):
        part_of = pl.ds(g * N // WG, N // WG)
        pltpu.make_async_copy(wq_h.at[part_of], wql.at[part_of], wqsem.at[g]).wait()

        @pl.loop(g * N // WG, (g + 1) * N // WG)
        def _(k):
            eq.over_z(k)

    kacc[...] = jnp.zeros_like(kacc)
    qacc[...] = jnp.zeros_like(qacc)

    def project_kv(k):
        token_arrived(k, ROWS, t2r)

        @pl.when(lax.rem(k, N // NK) == 0)
        def _():
            ek.ready(k // (N // NK))

        rows = pl.ds(pl.multiple_of(lax.rem(k, N // NK) * CW, CW), CW)
        for shard, w in ((p.zh, wkl), (1 - p.zh, wkr)):
            kacc[shard] = kacc[shard] + jnp.dot(
                tok[k], w[k // (N // NK), rows, :], preferred_element_type=F32
            )

    def project_q(k):
        eq.ready(k)
        qacc[p.zh] = qacc[p.zh] + jnp.dot(tok[k], wql[k], preferred_element_type=F32)
        qacc[1 - p.zh] = qacc[1 - p.zh] + jnp.dot(tok[k], wqr[k], preferred_element_type=F32)

    def output_step(v):
        when_in(v + AHEAD, AHEAD, N, eo.over_z)
        eo.stages(v)

    def token_step(c):
        when_in(c + LEAD, 0, N, tokens_send)
        when_in(c, 0, N, tokens_forward)

    first = (p.zl == 0) & (p.core == 0)
    ups = p.y < 3
    downs = (p.y == 0) | (p.y > 1)
    hops = (p.y, lax.rem(4 - p.y, 4))

    def pol_move(way, m, dev):
        rcopy(pol.at[m], pol.at[m], psent.at[way], pr.at[m], dev).start()

    def pol_arrived(m):
        rcopy(pol.at[m], pol.at[m], psem, pr.at[m], p.sib).wait_recv()

    def pol_step(j):
        @pl.when(root & (j == POL))
        def _():
            load_pol.wait()

        for d in (0, 1):
            t = j - POL - LAG * hops[d]
            m = PCH // 2 * d + t

            @pl.when(first & (t >= 0) & (t < PCH // 2))
            def _():
                @pl.when(p.y > 0)
                def _():
                    pol_arrived(m)

                @pl.when(downs if d else ups)
                def _():
                    pol_move(d, m, p.yl if d else p.yr)

                pol_move(2, m, p.zpart)
                pol_move(3, m, p.sib)

            t2 = t - LAG
            m2 = PCH // 2 * d + t2

            @pl.when((p.zl == 1) & (p.core == 0) & (t2 >= 0) & (t2 < PCH // 2))
            def _():
                pol_arrived(m2)
                pol_move(3, m2, p.sib)

    slot = p.x // 2
    near = lax.rem(p.x, 2)
    here = pl.ds(pl.multiple_of(p.zh * PLANE, PLANE), PLANE)
    pair0 = 2 * near
    nearest = pair0 + slot

    def kv_in_plane(kind, off):
        to = p.zh * 4 + pair0 + off
        return to, rcopy(
            kvs.at[kind], kva.at[kind, slot, here], ks.at[kind, off], kr.at[kind, slot * 2 + p.zh],
            (p.rep, to),
        )

    def kv_up(kind):
        return rcopy(
            kvs.at[kind], kva.at[kind, slot, here], ks.at[kind, 2], kr.at[kind, slot * 2],
            (p.rep, 4 + nearest),
        )

    def kv_beside(kind):
        ref = kva.at[kind, near, pl.ds(0, PLANE)]
        return rcopy(
            ref, ref, ks.at[kind, 2], kr.at[kind, near * 2], (p.rep, 4 + p.x + 1 - 2 * near)
        )

    def kv_wait(kind, j, pz):
        ref = kva.at[kind, j, pl.ds(pz * PLANE, PLANE)]
        rcopy(ref, ref, ks.at[0, 0], kr.at[kind, j * 2 + pz], p.sib).wait_recv()

    def kv_send():
        for kind in (0, 1):
            kvs[kind] = kacc[kind].astype(BF)

        @pl.when(p.zh == 0)
        def _():
            for kind in (0, 1):
                kv_up(kind).start()

        for kind in (0, 1):
            for off in (0, 1):
                to, copy = kv_in_plane(kind, off)

                @pl.when(to != p.tp)
                def _():
                    copy.start()

                @pl.when(to == p.tp)
                def _():
                    kva[kind, slot, here, :] = kvs[kind]

    @pl.loop(0, GAP)
    def _(i):
        c, off = 2 * i // 3, lax.rem(2 * i, 3)

        @pl.when(off != 2)
        def _():
            token_step(c)

        @pl.when(i == O0 - AHEAD)
        def _():
            pltpu.make_async_copy(wol, wol, wosem).wait()

        when_in(i - O0 + AHEAD, 0, AHEAD, eo.over_z)
        ek.stages(i)
        eq.stages(i)

        @pl.when((i >= O0) & (lax.rem(i - O0, SLOW) == 0))
        def _():
            output_step((i - O0) // SLOW)

        when_in(i - EP, 0, N, project_kv)

        @pl.when(i == EP + N - 1)
        def _():
            kv_send()

        when_in(i - Q0 - EP, 0, N, project_q)

    for s in (0, 1):
        qv[s] = qacc[s].astype(BF)

    @pl.when(p.zh == 1)
    def _():
        for kind in (0, 1):
            kv_wait(kind, near, 0)
            kv_beside(kind).start()

    def kv_arrived(kind, j, plane):
        @pl.when(2 * j + p.x // 2 != p.x)
        def _():
            kv_wait(kind, j, plane)

        if plane == 1:
            @pl.when(j != near)
            def _():
                kv_wait(kind, j, 0)

    last = length[0]

    def attend(turn, planes):
        keys = planes * PLANE
        rowpos = lax.broadcasted_iota(jnp.int32, (PLANE, keys), 0) + (planes - 1) * PLANE
        colpos = lax.broadcasted_iota(jnp.int32, (PLANE, keys), 1)
        valid = (colpos <= rowpos) & (colpos < last)
        s = near if turn == 0 else 1 - near
        heads = [slice(h * HS, (h + 1) * HS) for h in range(4)]
        kv_arrived(0, s, planes - 1)
        scores = [
            lax.dot_general(
                qv[s, :, cols], kva[0, s, :keys, :], (((1,), (1,)), ((), ())),
                preferred_element_type=F32,
            )
            for cols in heads
        ]
        scores = [jnp.where(valid, one, -1e30) for one in scores]
        tops = [jnp.max(one, axis=-1, keepdims=True) for one in scores]
        weights = [
            jnp.exp2((one - top) * (HS ** (-0.5) * 1.4426950408889634)) for one, top in zip(scores, tops)
        ]
        probs = [
            (one * (1.0 / jnp.sum(one, axis=-1, keepdims=True))).astype(BF) for one in weights
        ]
        kv_arrived(1, s, planes - 1)
        for cols, one in zip(heads, probs):
            att[s, :, cols] = jnp.dot(one, kva[1, s, :keys, :], preferred_element_type=F32).astype(BF)

    for turn in (0, 1):
        for plane in (0, 1):
            @pl.when(p.zh == plane)
            def _():
                attend(turn, plane + 1)
        if turn == 0:
            output_step(jnp.int32(V0))

    HALF = CW // 2

    def out_project(c):
        eo.ready(c)
        part[c] = (
            jnp.dot(att[p.zh], wol[c], preferred_element_type=F32)
            + jnp.dot(att[1 - p.zh], wor[c], preferred_element_type=F32)
        ).astype(BF)
        for d, dev in enumerate((p.xr, p.xl)):
            src = part.at[c, block(p.xo), pl.ds(d * HALF, HALF)]
            rcopy(src, r1.at[c, d], ssent, s1r.at[c], dev).start()

    def pass_on(c):
        rcopy(r1.at[c], r1.at[c], ssent, s1r.at[c], p.sib).wait_recv()
        for d, dev in enumerate((p.xr, p.xl)):
            rows, cols = block(p.xm if d else p.xp), pl.ds(d * HALF, HALF)
            part[c, rows, cols] = (part[c, rows, cols].astype(F32) + r1[c, d].astype(F32)).astype(BF)
            rcopy(part.at[c, rows], r2.at[c, d], ssent, s2r.at[c], dev).start()

    def finish(c):
        rcopy(r2.at[c], r2.at[c], ssent, s2r.at[c], p.sib).wait_recv()
        at = pl.ds(pl.multiple_of(c * CW, CW), CW)
        summed = part[c, own, :].astype(F32) + r2[c, 0].astype(F32) + r2[c, 1].astype(F32)
        out = (rv[c].astype(F32) + summed).astype(BF)
        hid[c] = out
        racc[...] = racc[...] + out.astype(F32) * head[at].astype(F32).reshape(1, CW)
        pltpu.make_async_copy(hid.at[c], hid_o.at[:, at], hsem).start()

    racc[...] = jnp.zeros_like(racc)

    @pl.loop(0, max(N + 2 * RL, POL + PCH // 2 + 4 * LAG))
    def _(it):
        when_in(it - RL, 0, N, pass_on)
        when_in(it, 0, N, out_project)
        output_step(it + V0 + 1)
        when_in(it - 2 * RL, 0, N, finish)
        pol_step(it)

    @pl.when(p.core == 1)
    def _():
        for m in range(PCH):
            pol_arrived(m)

    store_pol = pltpu.make_async_copy(pol, pol_o, psem)
    store_pol.start()

    rows = jnp.sum(racc[...], axis=-1, keepdims=True)
    position = lax.broadcasted_iota(jnp.int32, (ROWS, 1), 0) + p.tp * ROWS
    picked = jnp.where(position == last - 1, 1.0, 0.0) + 512 ** (-0.5)
    share = jnp.sum(rows * picked, axis=0, keepdims=True)
    rsend[...] = jnp.broadcast_to(share, (8, 128))

    for t in range(8):
        @pl.when(t != p.tp)
        def _():
            rcopy(rsend, rrecv.at[p.tp], wsent, wrecv, (p.rep, t)).start()

        @pl.when(t == p.tp)
        def _():
            rrecv[t] = rsend[...]

    for exchange in (ek, eq, eo):
        exchange.drain()
    sent = tok.at[:, pl.ds(0, 3 * ROWS)]
    rcopy(sent, sent, tsent, tsent, p.sib).wait_send()
    sent = part.at[:, pl.ds(0, 3 * ROWS)]
    rcopy(sent, sent, ssent, ssent, p.sib).wait_send()
    pltpu.make_async_copy(hid, hid, hsem).wait()

    for kind in (0, 1):
        for off in (0, 1):
            to, copy = kv_in_plane(kind, off)

            @pl.when(to != p.tp)
            def _():
                copy.wait_send()

        kv_up(kind).wait_send()

    def pol_sent(way, start, size):
        ref = pol.at[pl.ds(start, size)]
        rcopy(ref, ref, psent.at[way], psem, p.sib).wait_send()

    @pl.when(first & ups)
    def _():
        pol_sent(0, 0, PCH // 2)

    @pl.when(first & downs)
    def _():
        pol_sent(1, PCH // 2, PCH // 2)

    @pl.when(first)
    def _():
        pol_sent(2, 0, PCH)

    @pl.when(p.core == 0)
    def _():
        pol_sent(3, 0, PCH)

    sent = rrecv.at[pl.ds(0, 7)]
    rcopy(sent, sent, wsent, wrecv, p.sib).wait()
    rew_o[0] = jnp.max(jnp.sum(rrecv[...], axis=0))
    store_pol.wait()


def write_out(hid_i, pol_i, hid_o, pol_o, hbuf, pbuf, rsem, wsem):
    parts = 4
    copies = []
    for j, (src, buf, dst) in enumerate(((hid_i, hbuf, hid_o), (pol_i, pbuf, pol_o))):
        size = src.shape[0] // parts
        for m in range(parts):
            at, s = pl.ds(m * size, size), j * parts + m
            copies.append((
                pltpu.make_async_copy(src.at[at], buf.at[at], rsem.at[s]),
                pltpu.make_async_copy(buf.at[at], dst.at[at], wsem.at[s]),
            ))
    for read, _ in copies:
        read.start()
    for read, write in copies:
        read.wait()
        write.start()
    for _, write in copies:
        write.wait()


def on_device(residual_in, norm_gain, w_query, w_keyval, w_out, score_head, lengths, policy_slots):
    vmem = pl.BlockSpec(memory_space=pltpu.VMEM)
    smem = pl.BlockSpec(memory_space=pltpu.SMEM)
    hbm = pl.BlockSpec(memory_space=pl.ANY)
    dma = pltpu.SemaphoreType.DMA

    prow = policy_slots.shape[1]
    hidden, reward, policy = pl.pallas_call(
        kernel,
        out_shape=(
            jax.ShapeDtypeStruct((ROWS, D), BF),
            jax.ShapeDtypeStruct((1,), F32),
            jax.ShapeDtypeStruct((PCH, prow // PCH, 1024), BF),
        ),
        in_specs=[vmem, vmem, smem, hbm, hbm, hbm, hbm, hbm],
        out_specs=(hbm, smem, hbm),
        scratch_shapes=[
            pltpu.VMEM((N, ROWS, CW), BF),
            pltpu.VMEM((N, PLANE, CW), BF),
            pltpu.VMEM((NK, D // NK, KC), BF),
            pltpu.VMEM((NK, D // NK, KC), BF),
            pltpu.VMEM((N, CW, QC), BF),
            pltpu.VMEM((N, CW, QC), BF),
            pltpu.VMEM((N, QC, CW), BF),
            pltpu.VMEM((N, QC, CW), BF),
            pltpu.VMEM((2, PLANE, KC), F32),
            pltpu.VMEM((2, PLANE, QC), F32),
            pltpu.VMEM((2, PLANE, QC), BF),
            pltpu.VMEM((2, PLANE, HS), BF),
            pltpu.VMEM((2, 2, 2 * PLANE, HS), BF),
            pltpu.VMEM((2, PLANE, QC), BF),
            pltpu.VMEM((N, PLANE, CW), BF),
            pltpu.VMEM((N, 2, ROWS, CW // 2), BF),
            pltpu.VMEM((N, 2, ROWS, CW), BF),
            pltpu.VMEM((N, ROWS, CW), BF),
            pltpu.VMEM((ROWS, CW), F32),
            pltpu.VMEM((8, 128), F32),
            pltpu.VMEM((8, 8, 128), F32),
            pltpu.VMEM((PCH, prow // PCH, 1024), BF),
            dma, dma, dma((WG,)), dma, dma, dma((N,)), dma((N,)),
            dma, dma, dma, *[dma((NK + 2 * N,))] * 5,
            dma((2, 3)), dma((2, 4)), dma, dma((N,)), dma((N,)),
            dma, dma, dma, dma((4,)), dma((PCH,)), dma,
        ],
        compiler_params=pltpu.CompilerParams(
            collective_id=0, has_side_effects=True, vmem_limit_bytes=66_000_000
        ),
        name="block",
    )(
        norm_gain, score_head, lengths,
        residual_in[0], w_query.reshape(N, CW, QC), w_keyval.reshape(NK, D // NK, KC), w_out,
        policy_slots[0].reshape(PCH, prow // PCH, 1024),
    )
    hidden, policy = pl.pallas_call(
        write_out,
        out_shape=(
            jax.ShapeDtypeStruct(hidden.shape, BF),
            jax.ShapeDtypeStruct(policy.shape, BF),
        ),
        in_specs=[hbm, hbm],
        out_specs=(hbm, hbm),
        scratch_shapes=[pltpu.VMEM(hidden.shape, BF), pltpu.VMEM(policy.shape, BF), dma((8,)), dma((8,))],
        name="write_out",
    )(hidden, policy)
    return hidden[None], reward, policy.reshape(1, prow, 1024)


def solution(mesh):
    placed = (
        P("rep", "tp", None),
        P(),
        P(None, "tp"),
        P(None, "tp"),
        P("tp", None),
        P(),
        P("rep"),
        P("rep", None, "tp"),
    )
    return jax.shard_map(
        on_device,
        mesh=mesh,
        in_specs=placed,
        out_specs=(P("rep", "tp", None), P("rep"), P("rep", None, "tp")),
        check_vma=False,
    )
```

```python
import functools

import jax
import jax.numpy as jnp
from jax import lax
from jax.experimental import pallas as pl
from jax.experimental.pallas import tpu as pltpu
from jax.sharding import PartitionSpec as P

HS = 128
N = 16
D = 8192
CW = D // N
ROWS = 64
PLANE = 256
QC = 512
KC = 128
PCH = 16
NK = 4
E1, E2, E3, EP = 3, 6, 9, 10
KV0, Q0, O0 = 0, NK, NK + N
AHEAD = 4
GAP = NK + N + EP
SLOW = 1
V0 = -(-(GAP - O0) // SLOW)
LEAD = 3
RL, RF = 3, 4
POL = 5
LAG = 2
WG = 4
MESH = pl.DeviceIdType.MESH
BF = jnp.bfloat16
F32 = jnp.float32


def rcopy(src, dst, ssem, rsem, dev):
    return pltpu.make_async_remote_copy(
        src_ref=src, dst_ref=dst, send_sem=ssem, recv_sem=rsem, device_id=dev, device_id_type=MESH
    )


def when_in(value, low, high, fn):
    @pl.when((value >= low) & (value < high))
    def _():
        fn(value)


class Place:
    def __init__(self):
        rep = lax.axis_index("rep")
        tp = lax.axis_index("tp")
        self.rep, self.tp = rep, tp
        self.core = core = lax.rem(rep, 2)
        self.y = y = lax.rem(rep // 2, 4)
        self.zl = zl = rep // 8
        self.x = x = lax.rem(tp, 4)
        self.zh = zh = tp // 4
        self.xp, self.xm, self.xo = lax.rem(x + 1, 4), lax.rem(x + 3, 4), lax.rem(x + 2, 4)
        self.yp, self.ym, self.yo = lax.rem(y + 1, 4), lax.rem(y + 3, 4), lax.rem(y + 2, 4)
        self.xr = (rep, zh * 4 + self.xp)
        self.xl = (rep, zh * 4 + self.xm)
        self.yr = ((zl * 4 + self.yp) * 2 + core, tp)
        self.yl = ((zl * 4 + self.ym) * 2 + core, tp)
        self.cross = (((1 - zl) * 4 + y) * 2 + core, (1 - zh) * 4 + x)
        self.zpart = (((1 - zl) * 4 + y) * 2 + core, tp)
        self.sib = (rep + 1 - 2 * core, tp)


class Exchange:
    def __init__(self, p, near, far, first, base, sems):
        self.p, self.near, self.far, self.first, self.base = p, near, far, first, base
        self.count, self.rows = far.shape[:2]
        self.sent, self.cr, self.y1r, self.y2r, self.z2r, self.dr = sems

    def piece(self, yy, core, sub=0, subs=4):
        size = self.rows // 32
        start = yy * (self.rows // 4) + core * (self.rows // 8) + sub * size
        return pl.ds(pl.multiple_of(start, 16), subs * size)

    def move(self, k, where, rsem, dev):
        ref = self.far.at[k, where]
        rcopy(ref, ref, self.sent, rsem.at[self.base + k], dev).start()

    def arrived(self, k, count, rsem):
        ref = self.far.at[k, pl.ds(0, count * (self.rows // 32))]
        rcopy(ref, ref, self.sent, rsem.at[self.base + k], self.p.sib).wait_recv()

    def over_z(self, k):
        p = self.p
        where = self.piece(p.y, p.core)
        rcopy(
            self.near.at[k, where], self.far.at[k, where], self.sent, self.cr.at[self.base + k], p.cross
        ).start()

    def stage0(self, k):
        p = self.p
        self.arrived(k, 4, self.cr)
        self.move(k, self.piece(p.y, p.core, p.zl, 3), self.y1r, p.yr)
        self.move(k, self.piece(p.y, p.core, p.zl, 3), self.y1r, p.yl)
        self.move(k, self.piece(p.y, p.core), self.dr, p.sib)

    def stage1(self, k):
        p = self.p
        self.arrived(k, 6, self.y1r)
        self.move(k, self.piece(p.ym, p.core, 2 * p.zl, 1), self.y2r, p.yr)
        self.move(k, self.piece(p.yp, p.core, 2 * p.zl + 1, 1), self.y2r, p.yl)
        self.move(k, self.piece(p.ym, p.core, 3 * p.zl, 1), self.y2r, p.zpart)
        self.move(k, self.piece(p.yp, p.core, 3 * p.zl, 1), self.y2r, p.zpart)

    def stage2(self, k):
        p = self.p
        self.arrived(k, 4, self.y2r)
        self.move(k, self.piece(p.yo, p.core, 2 * p.zl, 2), self.z2r, p.zpart)
        self.move(k, self.piece(p.ym, p.core), self.dr, p.sib)
        self.move(k, self.piece(p.yp, p.core), self.dr, p.sib)

    def stage3(self, k):
        p = self.p
        self.arrived(k, 2, self.z2r)
        self.move(k, self.piece(p.yo, p.core), self.dr, p.sib)

    def ready(self, k):
        self.arrived(k, 16, self.dr)

    def stages(self, i):
        k = i - self.first
        when_in(k - E3, 0, self.count, self.stage3)
        when_in(k - E2, 0, self.count, self.stage2)
        when_in(k - E1, 0, self.count, self.stage1)
        when_in(k, 0, self.count, self.stage0)

    def drain(self):
        rcopy(self.far, self.far, self.sent, self.sent, self.p.sib).wait_send()


def kernel(
    gain, head, length, resid_h, wq_h, wkv_h, wo_h, pol_h,
    hid_o, rew_o, pol_o,
    rv, tok, wkl, wkr, wql, wqr, wol, wor, kacc, qacc, qv, kvs, kva, att, part, r1, r2, hid, racc, rsend, rrecv, pol,
    lsem, wksem, wqsem, wosem, tsent, t1r, t2r,
    ksent, qsent, osent, cr, y1r, y2r, z2r, dr,
    ks, kr, ssent, s1r, s2r, hsem, wsent, wrecv, psent, pr, psem,
):
    p = Place()
    recvs = (cr, y1r, y2r, z2r, dr)
    ek = Exchange(p, wkl, wkr, KV0, 0, (ksent, *recvs))
    eq = Exchange(p, wql, wqr, Q0, NK, (qsent, *recvs))
    eo = Exchange(p, wol, wor, 0, NK + N, (osent, *recvs))

    barrier = pltpu.get_barrier_semaphore()
    for t in range(8):
        @pl.when(t != p.tp)
        def _():
            pl.semaphore_signal(barrier, inc=1, device_id=(p.rep, t), device_id_type=MESH)
    for dev in (p.yr, p.yl, p.cross, p.zpart, p.sib):
        pl.semaphore_signal(barrier, inc=1, device_id=dev, device_id_type=MESH)

    root = (p.zl == 0) & (p.y == 0) & (p.core == 0)

    for k in range(N):
        pltpu.make_async_copy(resid_h.at[:, pl.ds(k * CW, CW)], rv.at[k], lsem).start()

    load_wk = pltpu.make_async_copy(wkv_h, wkl, wksem)
    load_wk.start()
    own = pl.ds(pl.multiple_of(p.x * ROWS, ROWS), ROWS)
    pltpu.make_async_copy(rv, rv, lsem).wait()
    for g in range(WG):
        part_of = pl.ds(g * N // WG, N // WG)
        pltpu.make_async_copy(wq_h.at[part_of], wql.at[part_of], wqsem.at[g]).start()

    @pl.loop(0, N)
    def _(k):
        at = pl.ds(pl.multiple_of(k * CW, CW), CW)
        pltpu.make_async_copy(wo_h.at[:, at], wol.at[k], wosem).start()

    load_pol = pltpu.make_async_copy(pol_h, pol, psem)

    @pl.when(root)
    def _():
        load_pol.start()

    squares = jnp.zeros((ROWS, 1), F32)
    for k in range(N):
        r = rv[k].astype(F32)
        squares += jnp.sum(r * r, axis=-1, keepdims=True)
    scale = lax.rsqrt(squares / D + 1e-05)
    for k in range(N):
        g = gain[k * CW : (k + 1) * CW].astype(F32).reshape(1, CW)
        tok[k, own, :] = (rv[k].astype(F32) * scale * g).astype(BF)

    pl.semaphore_wait(barrier, 12)

    def block(xx, start=0, size=ROWS):
        return pl.ds(pl.multiple_of(xx * ROWS + start, 16), size)

    def token_move(k, where, rsem, dev):
        ref = tok.at[k, where]
        rcopy(ref, ref, tsent, rsem.at[k], dev).start()

    def token_arrived(k, count, rsem):
        ref = tok.at[k, pl.ds(0, count)]
        rcopy(ref, ref, tsent, rsem.at[k], p.sib).wait_recv()

    def tokens_send(k):
        token_move(k, block(p.x), t1r, p.xr)
        token_move(k, block(p.x), t1r, p.xl)

    def tokens_forward(k):
        token_arrived(k, 2 * ROWS, t1r)
        token_move(k, block(p.xm, 0, 32), t2r, p.xr)
        token_move(k, block(p.xp, 32, 32), t2r, p.xl)

    for k in range(LEAD):
        tokens_send(k)

    load_wk.wait()
    for k in range(NK):
        ek.over_z(k)
    for g in range(WG):
        part_of = pl.ds(g * N // WG, N // WG)
        pltpu.make_async_copy(wq_h.at[part_of], wql.at[part_of], wqsem.at[g]).wait()

        @pl.loop(g * N // WG, (g + 1) * N // WG)
        def _(k):
            eq.over_z(k)

    kacc[...] = jnp.zeros_like(kacc)
    qacc[...] = jnp.zeros_like(qacc)

    def project_kv(k):
        token_arrived(k, ROWS, t2r)

        @pl.when(lax.rem(k, N // NK) == 0)
        def _():
            ek.ready(k // (N // NK))

        rows = pl.ds(pl.multiple_of(lax.rem(k, N // NK) * CW, CW), CW)
        for shard, w in ((p.zh, wkl), (1 - p.zh, wkr)):
            kacc[shard] = kacc[shard] + jnp.dot(
                tok[k], w[k // (N // NK), rows, :], preferred_element_type=F32
            )

    def project_q(k):
        eq.ready(k)
        qacc[p.zh] = qacc[p.zh] + jnp.dot(tok[k], wql[k], preferred_element_type=F32)
        qacc[1 - p.zh] = qacc[1 - p.zh] + jnp.dot(tok[k], wqr[k], preferred_element_type=F32)

    def output_step(v):
        when_in(v + AHEAD, AHEAD, N, eo.over_z)
        eo.stages(v)

    def token_step(c):
        when_in(c + LEAD, 0, N, tokens_send)
        when_in(c, 0, N, tokens_forward)

    first = (p.zl == 0) & (p.core == 0)
    ups = p.y < 3
    downs = (p.y == 0) | (p.y > 1)
    hops = (p.y, lax.rem(4 - p.y, 4))

    def pol_move(way, m, dev):
        rcopy(pol.at[m], pol.at[m], psent.at[way], pr.at[m], dev).start()

    def pol_arrived(m):
        rcopy(pol.at[m], pol.at[m], psem, pr.at[m], p.sib).wait_recv()

    def pol_step(j):
        @pl.when(root & (j == POL))
        def _():
            load_pol.wait()

        for d in (0, 1):
            t = j - POL - LAG * hops[d]
            m = PCH // 2 * d + t

            @pl.when(first & (t >= 0) & (t < PCH // 2))
            def _():
                @pl.when(p.y > 0)
                def _():
                    pol_arrived(m)

                @pl.when(downs if d else ups)
                def _():
                    pol_move(d, m, p.yl if d else p.yr)

                pol_move(2, m, p.zpart)
                pol_move(3, m, p.sib)

            t2 = t - LAG
            m2 = PCH // 2 * d + t2

            @pl.when((p.zl == 1) & (p.core == 0) & (t2 >= 0) & (t2 < PCH // 2))
            def _():
                pol_arrived(m2)
                pol_move(3, m2, p.sib)

    slot = p.x // 2
    near = lax.rem(p.x, 2)
    here = pl.ds(pl.multiple_of(p.zh * PLANE, PLANE), PLANE)
    pair0 = 2 * near
    nearest = pair0 + slot

    def kv_in_plane(kind, off):
        to = p.zh * 4 + pair0 + off
        return to, rcopy(
            kvs.at[kind], kva.at[kind, slot, here], ks.at[kind, off], kr.at[kind, slot * 2 + p.zh],
            (p.rep, to),
        )

    def kv_up(kind):
        return rcopy(
            kvs.at[kind], kva.at[kind, slot, here], ks.at[kind, 2], kr.at[kind, slot * 2],
            (p.rep, 4 + nearest),
        )

    def kv_beside(kind):
        ref = kva.at[kind, near, pl.ds(0, PLANE)]
        return rcopy(
            ref, ref, ks.at[kind, 2], kr.at[kind, near * 2], (p.rep, 4 + p.x + 1 - 2 * near)
        )

    def kv_wait(kind, j, pz):
        ref = kva.at[kind, j, pl.ds(pz * PLANE, PLANE)]
        rcopy(ref, ref, ks.at[0, 0], kr.at[kind, j * 2 + pz], p.sib).wait_recv()

    def kv_send():
        for kind in (0, 1):
            kvs[kind] = kacc[kind].astype(BF)

        @pl.when(p.zh == 0)
        def _():
            for kind in (0, 1):
                kv_up(kind).start()

        for kind in (0, 1):
            for off in (0, 1):
                to, copy = kv_in_plane(kind, off)

                @pl.when(to != p.tp)
                def _():
                    copy.start()

                @pl.when(to == p.tp)
                def _():
                    kva[kind, slot, here, :] = kvs[kind]

    @pl.loop(0, GAP)
    def _(i):
        c, off = 2 * i // 3, lax.rem(2 * i, 3)

        @pl.when(off != 2)
        def _():
            token_step(c)

        @pl.when(i == O0 - AHEAD)
        def _():
            pltpu.make_async_copy(wol, wol, wosem).wait()

        when_in(i - O0 + AHEAD, 0, AHEAD, eo.over_z)
        ek.stages(i)
        eq.stages(i)

        @pl.when((i >= O0) & (lax.rem(i - O0, SLOW) == 0))
        def _():
            output_step((i - O0) // SLOW)

        when_in(i - EP, 0, N, project_kv)

        @pl.when(i == EP + N - 1)
        def _():
            kv_send()

        when_in(i - Q0 - EP, 0, N, project_q)

    for s in (0, 1):
        qv[s] = qacc[s].astype(BF)

    @pl.when(p.zh == 1)
    def _():
        for kind in (0, 1):
            kv_wait(kind, near, 0)
            kv_beside(kind).start()

    def kv_arrived(kind, j, plane):
        @pl.when(2 * j + p.x // 2 != p.x)
        def _():
            kv_wait(kind, j, plane)

        if plane == 1:
            @pl.when(j != near)
            def _():
                kv_wait(kind, j, 0)

    last = length[0]

    def attend(turn, planes):
        keys = planes * PLANE
        rowpos = lax.broadcasted_iota(jnp.int32, (PLANE, keys), 0) + (planes - 1) * PLANE
        colpos = lax.broadcasted_iota(jnp.int32, (PLANE, keys), 1)
        valid = (colpos <= rowpos) & (colpos < last)
        s = near if turn == 0 else 1 - near
        heads = [slice(h * HS, (h + 1) * HS) for h in range(4)]
        kv_arrived(0, s, planes - 1)
        scores = [
            lax.dot_general(
                qv[s, :, cols], kva[0, s, :keys, :], (((1,), (1,)), ((), ())),
                preferred_element_type=F32,
            )
            for cols in heads
        ]
        scores = [jnp.where(valid, one, -1e30) for one in scores]
        tops = [jnp.max(one, axis=-1, keepdims=True) for one in scores]
        weights = [
            jnp.exp2((one - top) * (HS ** (-0.5) * 1.4426950408889634)) for one, top in zip(scores, tops)
        ]
        probs = [
            (one * (1.0 / jnp.sum(one, axis=-1, keepdims=True))).astype(BF) for one in weights
        ]
        kv_arrived(1, s, planes - 1)
        for cols, one in zip(heads, probs):
            att[s, :, cols] = jnp.dot(one, kva[1, s, :keys, :], preferred_element_type=F32).astype(BF)

    for turn in (0, 1):
        for plane in (0, 1):
            @pl.when(p.zh == plane)
            def _():
                attend(turn, plane + 1)
        if turn == 0:
            output_step(jnp.int32(V0))

    HALF = CW // 2

    def out_project(c):
        eo.ready(c)
        part[c] = (
            jnp.dot(att[p.zh], wol[c], preferred_element_type=F32)
            + jnp.dot(att[1 - p.zh], wor[c], preferred_element_type=F32)
        ).astype(BF)
        for d, dev in enumerate((p.xr, p.xl)):
            src = part.at[c, block(p.xo), pl.ds(d * HALF, HALF)]
            rcopy(src, r1.at[c, d], ssent, s1r.at[c], dev).start()

    def pass_on(c):
        rcopy(r1.at[c], r1.at[c], ssent, s1r.at[c], p.sib).wait_recv()
        for d, dev in enumerate((p.xr, p.xl)):
            rows, cols = block(p.xm if d else p.xp), pl.ds(d * HALF, HALF)
            part[c, rows, cols] = (part[c, rows, cols].astype(F32) + r1[c, d].astype(F32)).astype(BF)
            rcopy(part.at[c, rows], r2.at[c, d], ssent, s2r.at[c], dev).start()

    def finish(c):
        rcopy(r2.at[c], r2.at[c], ssent, s2r.at[c], p.sib).wait_recv()
        at = pl.ds(pl.multiple_of(c * CW, CW), CW)
        summed = part[c, own, :].astype(F32) + r2[c, 0].astype(F32) + r2[c, 1].astype(F32)
        out = (rv[c].astype(F32) + summed).astype(BF)
        hid[c] = out
        racc[...] = racc[...] + out.astype(F32) * head[at].astype(F32).reshape(1, CW)
        pltpu.make_async_copy(hid.at[c], hid_o.at[:, at], hsem).start()

    racc[...] = jnp.zeros_like(racc)

    @pl.loop(0, max(N + RL + RF, POL + PCH // 2 + 4 * LAG))
    def _(it):
        when_in(it - RL, 0, N, pass_on)
        when_in(it, 0, N, out_project)
        output_step(it + V0 + 1)
        when_in(it - RL - RF, 0, N, finish)
        pol_step(it)

    @pl.when(p.core == 1)
    def _():
        for m in range(PCH):
            pol_arrived(m)

    store_pol = pltpu.make_async_copy(pol, pol_o, psem)
    store_pol.start()

    rows = jnp.sum(racc[...], axis=-1, keepdims=True)
    position = lax.broadcasted_iota(jnp.int32, (ROWS, 1), 0) + p.tp * ROWS
    picked = jnp.where(position == last - 1, 1.0, 0.0) + 512 ** (-0.5)
    share = jnp.sum(rows * picked, axis=0, keepdims=True)
    rsend[...] = jnp.broadcast_to(share, (8, 128))

    for t in range(8):
        @pl.when(t != p.tp)
        def _():
            rcopy(rsend, rrecv.at[p.tp], wsent, wrecv, (p.rep, t)).start()

        @pl.when(t == p.tp)
        def _():
            rrecv[t] = rsend[...]

    for exchange in (ek, eq, eo):
        exchange.drain()
    sent = tok.at[:, pl.ds(0, 3 * ROWS)]
    rcopy(sent, sent, tsent, tsent, p.sib).wait_send()
    sent = part.at[:, pl.ds(0, 3 * ROWS)]
    rcopy(sent, sent, ssent, ssent, p.sib).wait_send()
    pltpu.make_async_copy(hid, hid, hsem).wait()

    for kind in (0, 1):
        for off in (0, 1):
            to, copy = kv_in_plane(kind, off)

            @pl.when(to != p.tp)
            def _():
                copy.wait_send()

        kv_up(kind).wait_send()

    def pol_sent(way, start, size):
        ref = pol.at[pl.ds(start, size)]
        rcopy(ref, ref, psent.at[way], psem, p.sib).wait_send()

    @pl.when(first & ups)
    def _():
        pol_sent(0, 0, PCH // 2)

    @pl.when(first & downs)
    def _():
        pol_sent(1, PCH // 2, PCH // 2)

    @pl.when(first)
    def _():
        pol_sent(2, 0, PCH)

    @pl.when(p.core == 0)
    def _():
        pol_sent(3, 0, PCH)

    sent = rrecv.at[pl.ds(0, 7)]
    rcopy(sent, sent, wsent, wrecv, p.sib).wait()
    rew_o[0] = jnp.max(jnp.sum(rrecv[...], axis=0))
    store_pol.wait()


def write_out(hid_i, pol_i, rew_i, hid_o, pol_o, rew_o, hbuf, pbuf, rbuf, rsem, wsem):
    parts = 4
    copies = []
    for j, (src, buf, dst) in enumerate(((hid_i, hbuf, hid_o), (pol_i, pbuf, pol_o))):
        size = src.shape[0] // parts
        for m in range(parts):
            at, s = pl.ds(m * size, size), j * parts + m
            copies.append((
                pltpu.make_async_copy(src.at[at], buf.at[at], rsem.at[s]),
                pltpu.make_async_copy(buf.at[at], dst.at[at], wsem.at[s]),
            ))
    copies.append((
        pltpu.make_async_copy(rew_i, rbuf, rsem.at[2 * parts]),
        pltpu.make_async_copy(rbuf, rew_o, wsem.at[2 * parts]),
    ))
    for read, _ in copies:
        read.start()
    for read, write in copies:
        read.wait()
        write.start()
    for _, write in copies:
        write.wait()


def on_device(residual_in, norm_gain, w_query, w_keyval, w_out, score_head, lengths, policy_slots):
    vmem = pl.BlockSpec(memory_space=pltpu.VMEM)
    smem = pl.BlockSpec(memory_space=pltpu.SMEM)
    hbm = pl.BlockSpec(memory_space=pl.ANY)
    dma = pltpu.SemaphoreType.DMA

    prow = policy_slots.shape[1]
    hidden, reward, policy = pl.pallas_call(
        kernel,
        out_shape=(
            jax.ShapeDtypeStruct((ROWS, D), BF),
            jax.ShapeDtypeStruct((1,), F32),
            jax.ShapeDtypeStruct((PCH, prow // PCH, 1024), BF),
        ),
        in_specs=[vmem, vmem, smem, hbm, hbm, hbm, hbm, hbm],
        out_specs=(hbm, smem, hbm),
        scratch_shapes=[
            pltpu.VMEM((N, ROWS, CW), BF),
            pltpu.VMEM((N, PLANE, CW), BF),
            pltpu.VMEM((NK, D // NK, KC), BF),
            pltpu.VMEM((NK, D // NK, KC), BF),
            pltpu.VMEM((N, CW, QC), BF),
            pltpu.VMEM((N, CW, QC), BF),
            pltpu.VMEM((N, QC, CW), BF),
            pltpu.VMEM((N, QC, CW), BF),
            pltpu.VMEM((2, PLANE, KC), F32),
            pltpu.VMEM((2, PLANE, QC), F32),
            pltpu.VMEM((2, PLANE, QC), BF),
            pltpu.VMEM((2, PLANE, HS), BF),
            pltpu.VMEM((2, 2, 2 * PLANE, HS), BF),
            pltpu.VMEM((2, PLANE, QC), BF),
            pltpu.VMEM((N, PLANE, CW), BF),
            pltpu.VMEM((N, 2, ROWS, CW // 2), BF),
            pltpu.VMEM((N, 2, ROWS, CW), BF),
            pltpu.VMEM((N, ROWS, CW), BF),
            pltpu.VMEM((ROWS, CW), F32),
            pltpu.VMEM((8, 128), F32),
            pltpu.VMEM((8, 8, 128), F32),
            pltpu.VMEM((PCH, prow // PCH, 1024), BF),
            dma, dma, dma((WG,)), dma, dma, dma((N,)), dma((N,)),
            dma, dma, dma, *[dma((NK + 2 * N,))] * 5,
            dma((2, 3)), dma((2, 4)), dma, dma((N,)), dma((N,)),
            dma, dma, dma, dma((4,)), dma((PCH,)), dma,
        ],
        compiler_params=pltpu.CompilerParams(
            collective_id=0, has_side_effects=True, vmem_limit_bytes=66_000_000
        ),
        name="block",
    )(
        norm_gain, score_head, lengths,
        residual_in[0], w_query.reshape(N, CW, QC), w_keyval.reshape(NK, D // NK, KC), w_out,
        policy_slots[0].reshape(PCH, prow // PCH, 1024),
    )
    hidden, policy, reward = pl.pallas_call(
        write_out,
        out_shape=(
            jax.ShapeDtypeStruct(hidden.shape, BF),
            jax.ShapeDtypeStruct(policy.shape, BF),
            jax.ShapeDtypeStruct(reward.shape, F32),
        ),
        in_specs=[hbm, hbm, hbm],
        out_specs=(hbm, hbm, hbm),
        scratch_shapes=[
            pltpu.VMEM(hidden.shape, BF), pltpu.VMEM(policy.shape, BF), pltpu.SMEM((1,), F32),
            dma((9,)), dma((9,)),
        ],
        name="write_out",
    )(hidden, policy, reward)
    return hidden[None], reward, policy.reshape(1, prow, 1024)


def solution(mesh):
    placed = (
        P("rep", "tp", None),
        P(),
        P(None, "tp"),
        P(None, "tp"),
        P("tp", None),
        P(),
        P("rep"),
        P("rep", None, "tp"),
    )
    return jax.shard_map(
        on_device,
        mesh=mesh,
        in_specs=placed,
        out_specs=(P("rep", "tp", None), P("rep"), P("rep", None, "tp")),
        check_vma=False,
    )
```

```python
import functools

import jax
import jax.numpy as jnp
from jax import lax
from jax.experimental import pallas as pl
from jax.experimental.pallas import tpu as pltpu
from jax.sharding import PartitionSpec as P

HS = 128
N = 16
D = 8192
CW = D // N
ROWS = 64
PLANE = 256
QC = 512
KC = 128
PCH = 16
NK = 4
E1, E2, E3, EP = 3, 6, 9, 10
KV0, Q0, O0 = 0, NK, NK + N
AHEAD = 5
GAP = NK + N + EP
SLOW = 1
V0 = -(-(GAP - O0) // SLOW)
LEAD = 3
RL, RF = 3, 4
POL = 6
LAG = 2
WG = 4
MESH = pl.DeviceIdType.MESH
BF = jnp.bfloat16
F32 = jnp.float32


def rcopy(src, dst, ssem, rsem, dev):
    return pltpu.make_async_remote_copy(
        src_ref=src, dst_ref=dst, send_sem=ssem, recv_sem=rsem, device_id=dev, device_id_type=MESH
    )


def when_in(value, low, high, fn):
    @pl.when((value >= low) & (value < high))
    def _():
        fn(value)


class Place:
    def __init__(self):
        rep = lax.axis_index("rep")
        tp = lax.axis_index("tp")
        self.rep, self.tp = rep, tp
        self.core = core = lax.rem(rep, 2)
        self.y = y = lax.rem(rep // 2, 4)
        self.zl = zl = rep // 8
        self.x = x = lax.rem(tp, 4)
        self.zh = zh = tp // 4
        self.xp, self.xm, self.xo = lax.rem(x + 1, 4), lax.rem(x + 3, 4), lax.rem(x + 2, 4)
        self.yp, self.ym, self.yo = lax.rem(y + 1, 4), lax.rem(y + 3, 4), lax.rem(y + 2, 4)
        self.xr = (rep, zh * 4 + self.xp)
        self.xl = (rep, zh * 4 + self.xm)
        self.yr = ((zl * 4 + self.yp) * 2 + core, tp)
        self.yl = ((zl * 4 + self.ym) * 2 + core, tp)
        self.cross = (((1 - zl) * 4 + y) * 2 + core, (1 - zh) * 4 + x)
        self.zpart = (((1 - zl) * 4 + y) * 2 + core, tp)
        self.sib = (rep + 1 - 2 * core, tp)


class Exchange:
    def __init__(self, p, near, far, first, base, sems):
        self.p, self.near, self.far, self.first, self.base = p, near, far, first, base
        self.count, self.rows = far.shape[:2]
        self.sent, self.cr, self.y1r, self.y2r, self.z2r, self.dr = sems

    def piece(self, yy, core, sub=0, subs=4):
        size = self.rows // 32
        start = yy * (self.rows // 4) + core * (self.rows // 8) + sub * size
        return pl.ds(pl.multiple_of(start, 16), subs * size)

    def move(self, k, where, rsem, dev):
        ref = self.far.at[k, where]
        rcopy(ref, ref, self.sent, rsem.at[self.base + k], dev).start()

    def arrived(self, k, count, rsem):
        ref = self.far.at[k, pl.ds(0, count * (self.rows // 32))]
        rcopy(ref, ref, self.sent, rsem.at[self.base + k], self.p.sib).wait_recv()

    def over_z(self, k):
        p = self.p
        where = self.piece(p.y, p.core)
        rcopy(
            self.near.at[k, where], self.far.at[k, where], self.sent, self.cr.at[self.base + k], p.cross
        ).start()

    def stage0(self, k):
        p = self.p
        self.arrived(k, 4, self.cr)
        self.move(k, self.piece(p.y, p.core, p.zl, 3), self.y1r, p.yr)
        self.move(k, self.piece(p.y, p.core, p.zl, 3), self.y1r, p.yl)
        self.move(k, self.piece(p.y, p.core), self.dr, p.sib)

    def stage1(self, k):
        p = self.p
        self.arrived(k, 6, self.y1r)
        self.move(k, self.piece(p.ym, p.core, 2 * p.zl, 1), self.y2r, p.yr)
        self.move(k, self.piece(p.yp, p.core, 2 * p.zl + 1, 1), self.y2r, p.yl)
        self.move(k, self.piece(p.ym, p.core, 3 * p.zl, 1), self.y2r, p.zpart)
        self.move(k, self.piece(p.yp, p.core, 3 * p.zl, 1), self.y2r, p.zpart)

    def stage2(self, k):
        p = self.p
        self.arrived(k, 4, self.y2r)
        self.move(k, self.piece(p.yo, p.core, 2 * p.zl, 2), self.z2r, p.zpart)
        self.move(k, self.piece(p.ym, p.core), self.dr, p.sib)
        self.move(k, self.piece(p.yp, p.core), self.dr, p.sib)

    def stage3(self, k):
        p = self.p
        self.arrived(k, 2, self.z2r)
        self.move(k, self.piece(p.yo, p.core), self.dr, p.sib)

    def ready(self, k):
        self.arrived(k, 16, self.dr)

    def stages(self, i):
        k = i - self.first
        when_in(k - E3, 0, self.count, self.stage3)
        when_in(k - E2, 0, self.count, self.stage2)
        when_in(k - E1, 0, self.count, self.stage1)
        when_in(k, 0, self.count, self.stage0)

    def drain(self):
        rcopy(self.far, self.far, self.sent, self.sent, self.p.sib).wait_send()


def kernel(
    gain, head, length, resid_h, wq_h, wkv_h, wo_h, pol_h,
    hid_o, rew_o, pol_o,
    rv, tok, wkl, wkr, wql, wqr, wol, wor, kacc, qacc, qv, kvs, kva, att, part, r1, r2, hid, racc, rsend, rrecv, pol,
    lsem, wksem, wqsem, wosem, tsent, t1r, t2r,
    ksent, qsent, osent, cr, y1r, y2r, z2r, dr,
    ks, kr, ssent, s1r, s2r, hsem, wsent, wrecv, psent, pr, psem,
):
    p = Place()
    recvs = (cr, y1r, y2r, z2r, dr)
    ek = Exchange(p, wkl, wkr, KV0, 0, (ksent, *recvs))
    eq = Exchange(p, wql, wqr, Q0, NK, (qsent, *recvs))
    eo = Exchange(p, wol, wor, 0, NK + N, (osent, *recvs))

    barrier = pltpu.get_barrier_semaphore()
    for t in range(8):
        @pl.when(t != p.tp)
        def _():
            pl.semaphore_signal(barrier, inc=1, device_id=(p.rep, t), device_id_type=MESH)
    for dev in (p.yr, p.yl, p.cross, p.zpart, p.sib):
        pl.semaphore_signal(barrier, inc=1, device_id=dev, device_id_type=MESH)

    root = (p.zl == 0) & (p.y == 0) & (p.core == 0)

    for k in range(N):
        pltpu.make_async_copy(resid_h.at[:, pl.ds(k * CW, CW)], rv.at[k], lsem).start()

    load_wk = pltpu.make_async_copy(wkv_h, wkl, wksem)
    load_wk.start()
    own = pl.ds(pl.multiple_of(p.x * ROWS, ROWS), ROWS)
    pltpu.make_async_copy(rv, rv, lsem).wait()
    for g in range(WG):
        part_of = pl.ds(g * N // WG, N // WG)
        pltpu.make_async_copy(wq_h.at[part_of], wql.at[part_of], wqsem.at[g]).start()

    @pl.loop(0, N)
    def _(k):
        at = pl.ds(pl.multiple_of(k * CW, CW), CW)
        pltpu.make_async_copy(wo_h.at[:, at], wol.at[k], wosem).start()

    load_pol = pltpu.make_async_copy(pol_h, pol, psem)

    @pl.when(root)
    def _():
        load_pol.start()

    squares = jnp.zeros((ROWS, 1), F32)
    for k in range(N):
        r = rv[k].astype(F32)
        squares += jnp.sum(r * r, axis=-1, keepdims=True)
    scale = lax.rsqrt(squares / D + 1e-05)
    for k in range(N):
        g = gain[k * CW : (k + 1) * CW].astype(F32).reshape(1, CW)
        tok[k, own, :] = (rv[k].astype(F32) * scale * g).astype(BF)

    pl.semaphore_wait(barrier, 12)

    def block(xx, start=0, size=ROWS):
        return pl.ds(pl.multiple_of(xx * ROWS + start, 16), size)

    def token_move(k, where, rsem, dev):
        ref = tok.at[k, where]
        rcopy(ref, ref, tsent, rsem.at[k], dev).start()

    def token_arrived(k, count, rsem):
        ref = tok.at[k, pl.ds(0, count)]
        rcopy(ref, ref, tsent, rsem.at[k], p.sib).wait_recv()

    def tokens_send(k):
        token_move(k, block(p.x), t1r, p.xr)
        token_move(k, block(p.x), t1r, p.xl)

    def tokens_forward(k):
        token_arrived(k, 2 * ROWS, t1r)
        token_move(k, block(p.xm, 0, 32), t2r, p.xr)
        token_move(k, block(p.xp, 32, 32), t2r, p.xl)

    for k in range(LEAD):
        tokens_send(k)

    load_wk.wait()
    for k in range(NK):
        ek.over_z(k)
    for g in range(WG):
        part_of = pl.ds(g * N // WG, N // WG)
        pltpu.make_async_copy(wq_h.at[part_of], wql.at[part_of], wqsem.at[g]).wait()

        @pl.loop(g * N // WG, (g + 1) * N // WG)
        def _(k):
            eq.over_z(k)

    kacc[...] = jnp.zeros_like(kacc)
    qacc[...] = jnp.zeros_like(qacc)

    def project_kv(k):
        token_arrived(k, ROWS, t2r)

        @pl.when(lax.rem(k, N // NK) == 0)
        def _():
            ek.ready(k // (N // NK))

        rows = pl.ds(pl.multiple_of(lax.rem(k, N // NK) * CW, CW), CW)
        for shard, w in ((p.zh, wkl), (1 - p.zh, wkr)):
            kacc[shard] = kacc[shard] + jnp.dot(
                tok[k], w[k // (N // NK), rows, :], preferred_element_type=F32
            )

    def project_q(k):
        eq.ready(k)
        qacc[p.zh] = qacc[p.zh] + jnp.dot(tok[k], wql[k], preferred_element_type=F32)
        qacc[1 - p.zh] = qacc[1 - p.zh] + jnp.dot(tok[k], wqr[k], preferred_element_type=F32)

    def output_step(v):
        when_in(v + AHEAD, AHEAD, N, eo.over_z)
        eo.stages(v)

    def token_step(c):
        when_in(c + LEAD, 0, N, tokens_send)
        when_in(c, 0, N, tokens_forward)

    first = (p.zl == 0) & (p.core == 0)
    ups = p.y < 3
    downs = (p.y == 0) | (p.y > 1)
    hops = (p.y, lax.rem(4 - p.y, 4))

    def pol_move(way, m, dev):
        rcopy(pol.at[m], pol.at[m], psent.at[way], pr.at[m], dev).start()

    def pol_arrived(m):
        rcopy(pol.at[m], pol.at[m], psem, pr.at[m], p.sib).wait_recv()

    def pol_step(j):
        @pl.when(root & (j == POL))
        def _():
            load_pol.wait()

        for d in (0, 1):
            t = j - POL - LAG * hops[d]
            m = PCH // 2 * d + t

            @pl.when(first & (t >= 0) & (t < PCH // 2))
            def _():
                @pl.when(p.y > 0)
                def _():
                    pol_arrived(m)

                @pl.when(downs if d else ups)
                def _():
                    pol_move(d, m, p.yl if d else p.yr)

                pol_move(2, m, p.zpart)
                pol_move(3, m, p.sib)

            t2 = t - LAG
            m2 = PCH // 2 * d + t2

            @pl.when((p.zl == 1) & (p.core == 0) & (t2 >= 0) & (t2 < PCH // 2))
            def _():
                pol_arrived(m2)
                pol_move(3, m2, p.sib)

    slot = p.x // 2
    near = lax.rem(p.x, 2)
    here = pl.ds(pl.multiple_of(p.zh * PLANE, PLANE), PLANE)
    pair0 = 2 * near
    nearest = pair0 + slot

    def kv_in_plane(kind, off):
        to = p.zh * 4 + pair0 + off
        return to, rcopy(
            kvs.at[kind], kva.at[kind, slot, here], ks.at[kind, off], kr.at[kind, slot * 2 + p.zh],
            (p.rep, to),
        )

    def kv_up(kind):
        return rcopy(
            kvs.at[kind], kva.at[kind, slot, here], ks.at[kind, 2], kr.at[kind, slot * 2],
            (p.rep, 4 + nearest),
        )

    def kv_beside(kind):
        ref = kva.at[kind, near, pl.ds(0, PLANE)]
        return rcopy(
            ref, ref, ks.at[kind, 2], kr.at[kind, near * 2], (p.rep, 4 + p.x + 1 - 2 * near)
        )

    def kv_wait(kind, j, pz):
        ref = kva.at[kind, j, pl.ds(pz * PLANE, PLANE)]
        rcopy(ref, ref, ks.at[0, 0], kr.at[kind, j * 2 + pz], p.sib).wait_recv()

    def kv_send():
        for kind in (0, 1):
            kvs[kind] = kacc[kind].astype(BF)

        @pl.when(p.zh == 0)
        def _():
            for kind in (0, 1):
                kv_up(kind).start()

        for kind in (0, 1):
            for off in (0, 1):
                to, copy = kv_in_plane(kind, off)

                @pl.when(to != p.tp)
                def _():
                    copy.start()

                @pl.when(to == p.tp)
                def _():
                    kva[kind, slot, here, :] = kvs[kind]

    @pl.loop(0, GAP)
    def _(i):
        c, off = 2 * i // 3, lax.rem(2 * i, 3)

        @pl.when(off != 2)
        def _():
            token_step(c)

        @pl.when(i == O0 - AHEAD)
        def _():
            pltpu.make_async_copy(wol, wol, wosem).wait()

        when_in(i - O0 + AHEAD, 0, AHEAD, eo.over_z)
        ek.stages(i)
        eq.stages(i)

        @pl.when((i >= O0) & (lax.rem(i - O0, SLOW) == 0))
        def _():
            output_step((i - O0) // SLOW)

        when_in(i - EP, 0, N, project_kv)

        @pl.when(i == EP + N - 1)
        def _():
            kv_send()

        when_in(i - Q0 - EP, 0, N, project_q)

    for s in (0, 1):
        qv[s] = qacc[s].astype(BF)

    @pl.when(p.zh == 1)
    def _():
        for kind in (0, 1):
            kv_wait(kind, near, 0)
            kv_beside(kind).start()

    def kv_arrived(kind, j, plane):
        @pl.when(2 * j + p.x // 2 != p.x)
        def _():
            kv_wait(kind, j, plane)

        if plane == 1:
            @pl.when(j != near)
            def _():
                kv_wait(kind, j, 0)

    last = length[0]

    def attend(turn, planes):
        keys = planes * PLANE
        rowpos = lax.broadcasted_iota(jnp.int32, (PLANE, keys), 0) + (planes - 1) * PLANE
        colpos = lax.broadcasted_iota(jnp.int32, (PLANE, keys), 1)
        valid = (colpos <= rowpos) & (colpos < last)
        s = near if turn == 0 else 1 - near
        heads = [slice(h * HS, (h + 1) * HS) for h in range(4)]
        kv_arrived(0, s, planes - 1)
        scores = [
            lax.dot_general(
                qv[s, :, cols], kva[0, s, :keys, :], (((1,), (1,)), ((), ())),
                preferred_element_type=F32,
            )
            for cols in heads
        ]
        scores = [jnp.where(valid, one, -1e30) for one in scores]
        tops = [jnp.max(one, axis=-1, keepdims=True) for one in scores]
        weights = [
            jnp.exp2((one - top) * (HS ** (-0.5) * 1.4426950408889634)) for one, top in zip(scores, tops)
        ]
        probs = [
            (one * (1.0 / jnp.sum(one, axis=-1, keepdims=True))).astype(BF) for one in weights
        ]
        kv_arrived(1, s, planes - 1)
        for cols, one in zip(heads, probs):
            att[s, :, cols] = jnp.dot(one, kva[1, s, :keys, :], preferred_element_type=F32).astype(BF)

    for turn in (0, 1):
        for plane in (0, 1):
            @pl.when(p.zh == plane)
            def _():
                attend(turn, plane + 1)
        if turn == 0:
            output_step(jnp.int32(V0))

    HALF = CW // 2

    def out_project(c):
        eo.ready(c)
        part[c] = (
            jnp.dot(att[p.zh], wol[c], preferred_element_type=F32)
            + jnp.dot(att[1 - p.zh], wor[c], preferred_element_type=F32)
        ).astype(BF)
        for d, dev in enumerate((p.xr, p.xl)):
            src = part.at[c, block(p.xo), pl.ds(d * HALF, HALF)]
            rcopy(src, r1.at[c, d], ssent, s1r.at[c], dev).start()

    def pass_on(c):
        rcopy(r1.at[c], r1.at[c], ssent, s1r.at[c], p.sib).wait_recv()
        for d, dev in enumerate((p.xr, p.xl)):
            rows, cols = block(p.xm if d else p.xp), pl.ds(d * HALF, HALF)
            part[c, rows, cols] = (part[c, rows, cols].astype(F32) + r1[c, d].astype(F32)).astype(BF)
            rcopy(part.at[c, rows], r2.at[c, d], ssent, s2r.at[c], dev).start()

    def finish(c):
        rcopy(r2.at[c], r2.at[c], ssent, s2r.at[c], p.sib).wait_recv()
        at = pl.ds(pl.multiple_of(c * CW, CW), CW)
        summed = part[c, own, :].astype(F32) + r2[c, 0].astype(F32) + r2[c, 1].astype(F32)
        out = (rv[c].astype(F32) + summed).astype(BF)
        hid[c] = out
        racc[...] = racc[...] + out.astype(F32) * head[at].astype(F32).reshape(1, CW)
        pltpu.make_async_copy(hid.at[c], hid_o.at[:, at], hsem).start()

    racc[...] = jnp.zeros_like(racc)

    @pl.loop(0, max(N + RL + RF, POL + PCH // 2 + 4 * LAG))
    def _(it):
        when_in(it - RL, 0, N, pass_on)
        when_in(it, 0, N, out_project)
        output_step(it + V0 + 1)
        when_in(it - RL - RF, 0, N, finish)
        pol_step(it)

    @pl.when(p.core == 1)
    def _():
        for m in range(PCH):
            pol_arrived(m)

    store_pol = pltpu.make_async_copy(pol, pol_o, psem)
    store_pol.start()

    rows = jnp.sum(racc[...], axis=-1, keepdims=True)
    position = lax.broadcasted_iota(jnp.int32, (ROWS, 1), 0) + p.tp * ROWS
    picked = jnp.where(position == last - 1, 1.0, 0.0) + 512 ** (-0.5)
    share = jnp.sum(rows * picked, axis=0, keepdims=True)
    rsend[...] = jnp.broadcast_to(share, (8, 128))

    for t in range(8):
        @pl.when(t != p.tp)
        def _():
            rcopy(rsend, rrecv.at[p.tp], wsent, wrecv, (p.rep, t)).start()

        @pl.when(t == p.tp)
        def _():
            rrecv[t] = rsend[...]

    for exchange in (ek, eq, eo):
        exchange.drain()
    sent = tok.at[:, pl.ds(0, 3 * ROWS)]
    rcopy(sent, sent, tsent, tsent, p.sib).wait_send()
    sent = part.at[:, pl.ds(0, 3 * ROWS)]
    rcopy(sent, sent, ssent, ssent, p.sib).wait_send()
    pltpu.make_async_copy(hid, hid, hsem).wait()

    for kind in (0, 1):
        for off in (0, 1):
            to, copy = kv_in_plane(kind, off)

            @pl.when(to != p.tp)
            def _():
                copy.wait_send()

        kv_up(kind).wait_send()

    def pol_sent(way, start, size):
        ref = pol.at[pl.ds(start, size)]
        rcopy(ref, ref, psent.at[way], psem, p.sib).wait_send()

    @pl.when(first & ups)
    def _():
        pol_sent(0, 0, PCH // 2)

    @pl.when(first & downs)
    def _():
        pol_sent(1, PCH // 2, PCH // 2)

    @pl.when(first)
    def _():
        pol_sent(2, 0, PCH)

    @pl.when(p.core == 0)
    def _():
        pol_sent(3, 0, PCH)

    sent = rrecv.at[pl.ds(0, 7)]
    rcopy(sent, sent, wsent, wrecv, p.sib).wait()
    rew_o[0] = jnp.max(jnp.sum(rrecv[...], axis=0))
    store_pol.wait()


def write_out(hid_i, pol_i, rew_i, hid_o, pol_o, rew_o, hbuf, pbuf, rbuf, rsem, wsem):
    parts = 4
    copies = []
    for j, (src, buf, dst) in enumerate(((hid_i, hbuf, hid_o), (pol_i, pbuf, pol_o))):
        size = src.shape[0] // parts
        for m in range(parts):
            at, s = pl.ds(m * size, size), j * parts + m
            copies.append((
                pltpu.make_async_copy(src.at[at], buf.at[at], rsem.at[s]),
                pltpu.make_async_copy(buf.at[at], dst.at[at], wsem.at[s]),
            ))
    copies.append((
        pltpu.make_async_copy(rew_i, rbuf, rsem.at[2 * parts]),
        pltpu.make_async_copy(rbuf, rew_o, wsem.at[2 * parts]),
    ))
    for read, _ in copies:
        read.start()
    for read, write in copies:
        read.wait()
        write.start()
    for _, write in copies:
        write.wait()


def on_device(residual_in, norm_gain, w_query, w_keyval, w_out, score_head, lengths, policy_slots):
    vmem = pl.BlockSpec(memory_space=pltpu.VMEM)
    smem = pl.BlockSpec(memory_space=pltpu.SMEM)
    hbm = pl.BlockSpec(memory_space=pl.ANY)
    dma = pltpu.SemaphoreType.DMA

    prow = policy_slots.shape[1]
    hidden, reward, policy = pl.pallas_call(
        kernel,
        out_shape=(
            jax.ShapeDtypeStruct((ROWS, D), BF),
            jax.ShapeDtypeStruct((1,), F32),
            jax.ShapeDtypeStruct((PCH, prow // PCH, 1024), BF),
        ),
        in_specs=[vmem, vmem, smem, hbm, hbm, hbm, hbm, hbm],
        out_specs=(hbm, smem, hbm),
        scratch_shapes=[
            pltpu.VMEM((N, ROWS, CW), BF),
            pltpu.VMEM((N, PLANE, CW), BF),
            pltpu.VMEM((NK, D // NK, KC), BF),
            pltpu.VMEM((NK, D // NK, KC), BF),
            pltpu.VMEM((N, CW, QC), BF),
            pltpu.VMEM((N, CW, QC), BF),
            pltpu.VMEM((N, QC, CW), BF),
            pltpu.VMEM((N, QC, CW), BF),
            pltpu.VMEM((2, PLANE, KC), F32),
            pltpu.VMEM((2, PLANE, QC), F32),
            pltpu.VMEM((2, PLANE, QC), BF),
            pltpu.VMEM((2, PLANE, HS), BF),
            pltpu.VMEM((2, 2, 2 * PLANE, HS), BF),
            pltpu.VMEM((2, PLANE, QC), BF),
            pltpu.VMEM((N, PLANE, CW), BF),
            pltpu.VMEM((N, 2, ROWS, CW // 2), BF),
            pltpu.VMEM((N, 2, ROWS, CW), BF),
            pltpu.VMEM((N, ROWS, CW), BF),
            pltpu.VMEM((ROWS, CW), F32),
            pltpu.VMEM((8, 128), F32),
            pltpu.VMEM((8, 8, 128), F32),
            pltpu.VMEM((PCH, prow // PCH, 1024), BF),
            dma, dma, dma((WG,)), dma, dma, dma((N,)), dma((N,)),
            dma, dma, dma, *[dma((NK + 2 * N,))] * 5,
            dma((2, 3)), dma((2, 4)), dma, dma((N,)), dma((N,)),
            dma, dma, dma, dma((4,)), dma((PCH,)), dma,
        ],
        compiler_params=pltpu.CompilerParams(
            collective_id=0, has_side_effects=True, vmem_limit_bytes=66_000_000
        ),
        name="block",
    )(
        norm_gain, score_head, lengths,
        residual_in[0], w_query.reshape(N, CW, QC), w_keyval.reshape(NK, D // NK, KC), w_out,
        policy_slots[0].reshape(PCH, prow // PCH, 1024),
    )
    hidden, policy, reward = pl.pallas_call(
        write_out,
        out_shape=(
            jax.ShapeDtypeStruct(hidden.shape, BF),
            jax.ShapeDtypeStruct(policy.shape, BF),
            jax.ShapeDtypeStruct(reward.shape, F32),
        ),
        in_specs=[hbm, hbm, hbm],
        out_specs=(hbm, hbm, hbm),
        scratch_shapes=[
            pltpu.VMEM(hidden.shape, BF), pltpu.VMEM(policy.shape, BF), pltpu.SMEM((1,), F32),
            dma((9,)), dma((9,)),
        ],
        name="write_out",
    )(hidden, policy, reward)
    return hidden[None], reward, policy.reshape(1, prow, 1024)


def solution(mesh):
    placed = (
        P("rep", "tp", None),
        P(),
        P(None, "tp"),
        P(None, "tp"),
        P("tp", None),
        P(),
        P("rep"),
        P("rep", None, "tp"),
    )
    return jax.shard_map(
        on_device,
        mesh=mesh,
        in_specs=placed,
        out_specs=(P("rep", "tp", None), P("rep"), P("rep", None, "tp")),
        check_vma=False,
    )
```
